256 devices in a mesh: grp: 2 (over x_lo), blk: 128 (over x_hi, z, y, core).
Axes of the slice: x: 4 (x_hi: 2, x_lo: 2; x = x_hi * 2 + x_lo), y: 4, z: 8, core: 2. Of those that a mesh axis runs over, the one named last changes fastest.
Arguments:
- atoms: bfloat16 [131072, 512], P(('grp', 'blk')), parts along dimension 0, may hold values from -8 to 8
- edge_mask: int32 [256, 5, 512, 512], P(('grp', 'blk')), parts along dimension 0, may hold values from 0 to 1
- norm_gain: float32 [512], replicated, may hold values from 0.25 to 1.75
- w_query: bfloat16 [512, 512], replicated, may hold values from -3 to 3
- w_key: bfloat16 [512, 512], replicated, may hold values from -3 to 3
- w_value: bfloat16 [512, 512], replicated, may hold values from -0.25 to 0.25
- w_out: bfloat16 [512, 512], replicated, may hold values from -0.25 to 0.25
- bn_gain: float32 [512], replicated, may hold values from 0.25 to 1.75
- bn_shift: float32 [512], replicated, may hold values from -3 to 3
- w_up: bfloat16 [512, 1024], replicated, may hold values from -0.25 to 0.25
- w_down: bfloat16 [1024, 512], replicated, may hold values from -0.1875 to 0.1875
Outputs:
- updated: bfloat16 [131072, 512], P(('grp', 'blk')), parts along dimension 0
The draws below stay inside these ranges and needn't reach their ends.
There are 2 independent parts, one for each index of `grp`. The reference program is written for one: setup_inputs(seed, part) draws one part's arguments, and reference() takes and returns one part's arrays. A program takes and returns all parts, laid end to end along the dimension named above; an argument that names none is the same for every part. Nothing has to cross between parts.
All inputs are finite; a program needn't handle non-finite values.
Results may differ from the reference program's by a relative error of at most 0.01.
The reference program's roundings to bfloat16 on the way (of `normed`, `query`, `weight`, `mixed`, `batched` and `hidden`) count: a program that leaves them out, or rounds other values in their place, can miss the bound.
Values may be sent and summed in bfloat16 or wider, within the bound.
A program may use at most 128 MiB of HBM per device.

```python
import jax
import jax.numpy as jnp
from jax import lax

D = 512
HEADS = 8
HEAD_DIM = 64
FF = 1024
REACH = 2
TILE = 512
ATOMS = 65536


def draw_atoms(key, part):
    key_base = jax.random.fold_in(key, 11)
    key_one, key_two, key_three, key_four = jax.random.split(key_base, 4)
    ntiles = ATOMS // TILE
    tile_ids = (jnp.arange(ATOMS) // TILE).astype(jnp.int32)
    tile_index = tile_ids.astype(jnp.float32)
    rising = (1.0 + 2.0 * tile_index / (ntiles - 1))[:, None]
    parity = (1 - 2 * (tile_ids % 2)).astype(jnp.float32)[:, None]
    row_scale = jnp.exp(jax.random.uniform(key_two, (ATOMS, 1), jnp.float32, -0.69, 0.69))
    noise = jnp.clip(jax.random.normal(key_one, (ATOMS, D), jnp.float32), -6.0, 6.0)
    feature_mean = jnp.clip(jax.random.normal(key_three, (1, D), jnp.float32), -3.0, 3.0)
    bulk = noise * row_scale * rising + feature_mean * rising
    alternate = jnp.clip(jax.random.normal(key_four, (1, D), jnp.float32), -3.0, 3.0)
    return (0.1 * (bulk + alternate * parity)).astype(jnp.bfloat16)


def projection_draw(key, salt):
    base = jax.random.normal(jax.random.fold_in(key, salt), (D, D), jnp.float32)
    base = jnp.clip(base, -4.0, 4.0) * D ** (-0.5)
    return base.astype(jnp.bfloat16)


def draw_w_query(key, part):
    return projection_draw(key, 21)


def draw_w_key(key, part):
    return projection_draw(key, 22)


def draw_edge_mask(key, part):
    ntiles = ATOMS // TILE
    widths = 2 * REACH + 1
    key_base = jax.random.fold_in(key, 31)
    key_one, key_two, key_three = jax.random.split(key_base, 3)
    cut_level = jax.random.randint(key_one, (ntiles, widths, 1, 1), 0, 12)
    own_level = jax.random.randint(key_two, (ntiles, widths, 1, 1), 6, 24)
    offset = jnp.arange(widths).reshape(1, widths, 1, 1)
    level = jnp.where(offset == REACH, own_level, cut_level)
    draws = jax.random.randint(key_three, (ntiles, widths, TILE, TILE), 0, 64)
    return (draws < level).astype(jnp.int32)


def centred(key, extent, scale, reach, dtype=jnp.bfloat16):
    values = scale * jax.random.normal(key, extent, jnp.float32)
    return jnp.clip(values, min=-reach, max=reach).astype(dtype)


def setup_inputs(seed: int = 0, part: int = 0) -> dict:
    splits = jax.random.split(jax.random.key(seed), 12)
    part_keys = jax.random.split(jax.random.fold_in(splits[11], part), 12)
    return {
        "atoms": draw_atoms(jax.random.fold_in(jax.random.fold_in(splits[11], part), 71), part),
        "edge_mask": draw_edge_mask(jax.random.fold_in(jax.random.fold_in(splits[11], part), 71), part),
        "norm_gain": jnp.clip(1.0 + 0.15 * jax.random.normal(splits[2], (D,), jnp.float32), 0.25, 1.75),
        "w_query": draw_w_query(jax.random.fold_in(splits[11], 71), part),
        "w_key": draw_w_key(jax.random.fold_in(splits[11], 71), part),
        "w_value": centred(splits[5], (D, D), D ** -0.5, 0.25),
        "w_out": centred(splits[6], (D, D), D ** -0.5, 0.25),
        "bn_gain": jnp.clip(1.0 + 0.15 * jax.random.normal(splits[7], (D,), jnp.float32), 0.25, 1.75),
        "bn_shift": centred(splits[8], (D,), 0.5, 3.0, jnp.float32),
        "w_up": centred(splits[9], (D, FF), D ** -0.5, 0.25),
        "w_down": centred(splits[10], (FF, D), FF ** -0.5, 0.1875),
    }


def reference(atoms, edge_mask, norm_gain, w_query, w_key, w_value, w_out, bn_gain, bn_shift, w_up, w_down):
    ntiles = ATOMS // TILE
    widths = 2 * REACH + 1
    scale = HEAD_DIM ** (-0.5)
    xfull = atoms.astype(jnp.float32)
    normed = (xfull * lax.rsqrt(lax.optimization_barrier(jnp.mean(xfull * xfull, axis=-1, keepdims=True)) + 1e-06) * norm_gain).astype(jnp.bfloat16)
    query = jnp.dot(normed, w_query, preferred_element_type=jnp.float32).astype(jnp.bfloat16)
    keys = jnp.dot(normed, w_key, preferred_element_type=jnp.float32).astype(jnp.bfloat16)
    values = jnp.dot(normed, w_value, preferred_element_type=jnp.float32).astype(jnp.bfloat16)
    q_tiles = query.reshape(ntiles, TILE, HEADS, HEAD_DIM)
    k_tiles = keys.reshape(ntiles, TILE, HEADS, HEAD_DIM)
    v_tiles = values.reshape(ntiles, TILE, HEADS, HEAD_DIM)
    k_near = jnp.stack([jnp.roll(k_tiles, -(o - REACH), axis=0) for o in range(widths)], axis=1).reshape(ntiles, widths * TILE, HEADS, HEAD_DIM)
    v_near = jnp.stack([jnp.roll(v_tiles, -(o - REACH), axis=0) for o in range(widths)], axis=1).reshape(ntiles, widths * TILE, HEADS, HEAD_DIM)
    rows = lax.broadcasted_iota(jnp.int32, (TILE, widths, TILE), 0)
    cols = lax.broadcasted_iota(jnp.int32, (TILE, widths, TILE), 2)
    block = lax.broadcasted_iota(jnp.int32, (TILE, widths, TILE), 1)
    selfmask = ((rows == cols) & (block == REACH)).reshape(TILE, widths * TILE)

    def one_tile(pieces):
        qpart, kpart, vpart, mpart = pieces
        allowed = (jnp.transpose(mpart, (1, 0, 2)).reshape(TILE, widths * TILE) > 0) | selfmask
        score = jnp.einsum('qhd,khd->hqk', qpart.astype(jnp.float32), kpart.astype(jnp.float32)) * scale
        score = jnp.where(allowed[None], score, -1e+30)
        top = lax.optimization_barrier(jnp.max(score, axis=-1, keepdims=True))
        expo = jnp.exp(score - top)
        total = lax.optimization_barrier(jnp.sum(expo, axis=-1))
        weight = expo.astype(jnp.bfloat16)
        summed = jnp.einsum('hqk,khd->qhd', weight.astype(jnp.float32), vpart.astype(jnp.float32))
        return (summed / jnp.transpose(total)[:, :, None]).reshape(TILE, D).astype(jnp.bfloat16)
    mixed = lax.map(one_tile, (q_tiles, k_near, v_near, edge_mask)).reshape(ATOMS, D)
    after = xfull + jnp.dot(mixed, w_out, preferred_element_type=jnp.float32)
    mean = lax.optimization_barrier(jnp.mean(after, axis=0))
    var = lax.optimization_barrier(jnp.mean((after - mean) ** 2, axis=0))
    batched = ((after - mean) * lax.rsqrt(var + 1e-05) * bn_gain + bn_shift).astype(jnp.bfloat16)
    hidden = jax.nn.gelu(jnp.dot(batched, w_up, preferred_element_type=jnp.float32), approximate=True).astype(jnp.bfloat16)
    return (after + jnp.dot(hidden, w_down, preferred_element_type=jnp.float32)).astype(jnp.bfloat16)
```

```python
import functools
import math

import jax
import jax.numpy as jnp
from jax import lax
from jax.experimental import pallas as pl
from jax.experimental.pallas import tpu as pltpu
from jax.sharding import PartitionSpec as P

F32 = jnp.float32
BF16 = jnp.bfloat16
T = 512
D = 512
HEADS = 8
HEAD_DIM = 64
FF = 1024
SLABS = 5
VROWS = 80
AROWS = 72
CHUNKS = 2
CROWS = T // CHUNKS
NEG = -1e30
SCALE = HEAD_DIM**-0.5 * math.log2(math.e)
NY, NZ, NX = 4, 8, 2
PLANE = NX * NY * 2
BLOCKS = PLANE * NZ


def mm(a, b):
    return jnp.dot(a, b, preferred_element_type=F32)


def mm_nt(a, b):
    return lax.dot_general(a, b, (((1,), (1,)), ((), ())), preferred_element_type=F32)


def kernel(
    atoms_hbm, mask_hbm, gain_hbm, wq_hbm, wk_hbm, wv_hbm, wo_hbm, bng_hbm, bns_hbm, wu_hbm, wd_hbm,
    out_hbm,
    atoms, mask, gain, wq, wk, wv, wo, bng, bns, wu, wd,
    nrm, recv, wqt, wvt, qz, keys, vals, bias, t0, t1, p0, p1, a0, a1, top, acc,
    mixed, after, result, stat, stat_a, stat_m, stat_b,
    load_sem, out_sem, own_send, own_recv, fst_send, fst_recv, fwd_send, fwd_recv, snd_send, snd_recv,
    sa_send, sa_recv, sb_send, sb_recv,
):
    me = lax.axis_index("blk")
    core = lax.rem(me, 2)
    y = lax.rem(me // 2, NY)
    z = lax.rem(me // (2 * NY), NZ)
    xh = me // (2 * NY * NZ)
    sgn = 1 - 2 * core
    partner = me + sgn
    ahead = lax.rem(me + 2 * sgn + BLOCKS, BLOCKS)
    behind = lax.rem(me - 2 * sgn + BLOCKS, BLOCKS)
    place = xh * (NY * 2) + y * 2 + core

    def plane_peer(j):
        u = lax.rem(place + j, PLANE)
        return ((u // (NY * 2)) * NZ + z) * (NY * 2) + lax.rem(u, NY * 2)

    def line_peer(j):
        return (xh * NZ + lax.rem(z + j, NZ)) * (NY * 2) + y * 2 + core

    offsets = [2, 2 + sgn, 2 + 2 * sgn, 2 - sgn, 2 - 2 * sgn]
    loads = [
        pltpu.make_async_copy(atoms_hbm, atoms, load_sem.at[0]),
        pltpu.make_async_copy(gain_hbm, gain, load_sem.at[1]),
        pltpu.make_async_copy(wq_hbm, wq, load_sem.at[2]),
        pltpu.make_async_copy(wk_hbm, wk, load_sem.at[3]),
        pltpu.make_async_copy(wv_hbm, wv, load_sem.at[4]),
    ]
    mask_loads = [
        pltpu.make_async_copy(mask_hbm.at[0, offsets[s]], mask.at[s], load_sem.at[5 + s])
        for s in range(SLABS)
    ]
    late = [
        pltpu.make_async_copy(wo_hbm, wo, load_sem.at[10]),
        pltpu.make_async_copy(bng_hbm, bng, load_sem.at[11]),
        pltpu.make_async_copy(bns_hbm, bns, load_sem.at[12]),
        pltpu.make_async_copy(wu_hbm, wu, load_sem.at[13]),
        pltpu.make_async_copy(wd_hbm, wd, load_sem.at[14]),
    ]
    for copy in loads + mask_loads + late:
        copy.start()

    barrier = pltpu.get_barrier_semaphore()
    peers = [partner, ahead, behind]
    peers += [plane_peer(j) for j in range(1, PLANE)]
    peers += [line_peer(j) for j in range(1, NZ)]
    for peer in peers:
        pl.semaphore_signal(
            barrier, inc=1, device_id={"blk": peer}, device_id_type=pl.DeviceIdType.MESH
        )

    def remote(src, dst, send, rec, device):
        return pltpu.make_async_remote_copy(
            src_ref=src, dst_ref=dst, send_sem=send, recv_sem=rec,
            device_id={"blk": device}, device_id_type=pl.DeviceIdType.MESH,
        )

    def rows(c):
        return pl.ds(c * CROWS, CROWS)

    own = remote(nrm, recv.at[0], own_send, own_recv, partner)
    first = [
        remote(nrm.at[rows(c)], recv.at[1, rows(c)], fst_send.at[c], fst_recv.at[c], behind)
        for c in range(CHUNKS)
    ]
    passed = [
        remote(recv.at[1, rows(c)], recv.at[2, rows(c)], fwd_send.at[c], fwd_recv.at[c], partner)
        for c in range(CHUNKS)
    ]
    second = [
        remote(nrm.at[rows(c)], recv.at[3, rows(c)], snd_send.at[c], snd_recv.at[c], ahead)
        for c in range(CHUNKS)
    ]

    loads[0].wait()
    loads[1].wait()
    x = atoms[...].astype(F32)
    nrm[...] = (
        x * lax.rsqrt(jnp.mean(x * x, axis=-1, keepdims=True) + 1e-6) * gain[...]
    ).astype(BF16)
    pl.semaphore_wait(barrier, len(peers))
    for copy in first:
        copy.start()
    own.start()

    for copy in loads[2:]:
        copy.wait()
    wqt[...] = wq[...].T
    wvt[...] = wv[...].T

    def project(slot, features):
        k = mm(features, wk[...]).astype(BF16)
        for pair in range(HEADS // 2):
            keys[slot, pair] = k[:, pair * 128 : (pair + 1) * 128]
        v = mm_nt(wvt[...], features).astype(BF16)
        for h in range(HEADS):
            vals[slot, h, 0:HEAD_DIM] = v[h * HEAD_DIM : (h + 1) * HEAD_DIM]

    def make_bias(slot):
        mask_loads[slot].wait()
        for kc in range(T // 128):
            allowed = mask[slot, :, kc * 128 : (kc + 1) * 128] > 0
            if slot == 0:
                r = lax.broadcasted_iota(jnp.int32, (T, 128), 0)
                c = lax.broadcasted_iota(jnp.int32, (T, 128), 1) + kc * 128
                allowed = allowed | (r == c)
            bias[slot, kc * 128 : (kc + 1) * 128] = jnp.where(allowed, 0.0, NEG).astype(F32).T

    features = nrm[...]
    q = mm_nt(wqt[...], features).astype(BF16)
    zero = jnp.zeros((HEAD_DIM, T), BF16)
    for h in range(HEADS):
        part = q[h * HEAD_DIM : (h + 1) * HEAD_DIM]
        qz[h, 0:HEAD_DIM] = part if h % 2 == 0 else zero
        qz[h, HEAD_DIM : 2 * HEAD_DIM] = zero if h % 2 == 0 else part
    for s in range(SLABS):
        for h in range(HEADS):
            vals[s, h, HEAD_DIM:VROWS] = jnp.ones((VROWS - HEAD_DIM, T), BF16)
    project(0, features)
    make_bias(0)

    def score(slot, pair, h, t, a, fresh):
        best = None
        for kc in range(2):
            ks = slice(kc * 256, (kc + 1) * 256)
            s = mm(keys[slot, pair, ks], qz[h]) + bias[slot, ks]
            t[ks] = s
            m = jnp.max(s, axis=0, keepdims=True)
            best = m if best is None else jnp.maximum(best, m)
        if fresh:
            top[h] = jnp.broadcast_to(best, (8, T))
        else:
            old = top[h]
            new = jnp.maximum(old, best)
            a[...] = jnp.exp2((old - new) * SCALE)
            top[h] = new

    def weigh(h, t, p):
        m = top[h][0:1]
        for kc in range(4):
            ks = slice(kc * 128, (kc + 1) * 128)
            p[ks] = jnp.exp2((t[ks] - m) * SCALE).astype(BF16)

    def gather(slot, h, p, a, fresh):
        new = mm(vals[slot, h], p[...])[0:AROWS]
        if fresh:
            acc[h] = new
        else:
            acc[h] = acc[h] * a[0:1] + new

    def attend(slot, fresh=False):
        score(slot, 0, 0, t0, a0, fresh)
        score(slot, 0, 1, t1, a1, fresh)
        weigh(0, t0, p0)

        def step(j, carry):
            gather(slot, 2 * j - 2, p0, a0, fresh)
            weigh(2 * j - 1, t1, p1)
            score(slot, j, 2 * j, t0, a0, fresh)
            gather(slot, 2 * j - 1, p1, a1, fresh)
            weigh(2 * j, t0, p0)
            score(slot, j, 2 * j + 1, t1, a1, fresh)
            return carry

        lax.fori_loop(1, HEADS // 2, step, 0)
        weigh(HEADS - 1, t1, p1)
        gather(slot, HEADS - 2, p0, a0, fresh)
        gather(slot, HEADS - 1, p1, a1, fresh)

    attend(0, fresh=True)

    for copy in first:
        copy.wait_send()
    for copy in second:
        copy.start()
    first[0].wait_recv()
    passed[0].start()

    own.wait_recv()
    project(1, recv[0])
    make_bias(1)
    attend(1)

    for copy in first[1:]:
        copy.wait_recv()
    for copy in passed[1:]:
        copy.start()
    project(2, recv[1])
    make_bias(2)
    attend(2)

    for copy in passed:
        copy.wait_recv()
    project(3, recv[2])
    make_bias(3)
    attend(3)

    for copy in second:
        copy.wait_recv()
    project(4, recv[3])
    make_bias(4)
    attend(4)

    for h in range(HEADS):
        a = acc[h]
        mixed[h * HEAD_DIM : (h + 1) * HEAD_DIM] = (
            a[0:HEAD_DIM] / a[HEAD_DIM : HEAD_DIM + 1]
        ).astype(BF16)
    for copy in late:
        copy.wait()
    mix = mixed[...].T
    res = atoms[...].astype(F32) + mm(mix, wo[...])
    after[...] = res

    mean = jnp.sum(res, axis=0, keepdims=True) * (1.0 / T)
    dev = after[...] - mean
    m2 = jnp.sum(dev * dev, axis=0, keepdims=True)
    stat[0:1] = mean
    stat[1:2] = m2

    def merge(mean, m2, others, count, size):
        total = mean
        for j in range(1, count):
            total = total + others[j, 0:1]
        new = total * (1.0 / count)
        spread = (mean - new) * (mean - new)
        for j in range(1, count):
            d = others[j, 0:1] - new
            spread = spread + d * d
            m2 = m2 + others[j, 1:2]
        return new, m2 + spread * size

    plane = [
        remote(stat, stat_a.at[j], sa_send.at[j], sa_recv.at[j], plane_peer(j))
        for j in range(1, PLANE)
    ]
    for copy in plane:
        copy.start()
    for copy in plane:
        copy.wait_recv()
    mean, m2 = merge(mean, m2, stat_a, PLANE, float(T))
    stat_m[0:1] = mean
    stat_m[1:2] = m2
    line = [
        remote(stat_m, stat_b.at[j], sb_send.at[j], sb_recv.at[j], line_peer(j))
        for j in range(1, NZ)
    ]
    for copy in line:
        copy.start()
    for copy in line:
        copy.wait_recv()
    mean, m2 = merge(mean, m2, stat_b, NZ, float(T * PLANE))
    var = m2 * (1.0 / (T * BLOCKS))
    factor = lax.rsqrt(var + 1e-5) * bng[...]

    outs = []
    for c in range(2):
        rs = slice(c * 256, (c + 1) * 256)
        a = after[rs]
        batched = ((a - mean) * factor + bns[...]).astype(BF16)
        hidden = jax.nn.gelu(mm(batched, wu[...]), approximate=True).astype(BF16)
        result[rs] = (a + mm(hidden, wd[...])).astype(BF16)
        copy = pltpu.make_async_copy(result.at[rs], out_hbm.at[rs], out_sem.at[c])
        copy.start()
        outs.append(copy)

    own.wait_send()
    for copy in passed + second + plane + line:
        copy.wait_send()
    for copy in outs:
        copy.wait()


def body(atoms, edge_mask, norm_gain, w_query, w_key, w_value, w_out, bn_gain, bn_shift, w_up, w_down):
    dma = pltpu.SemaphoreType.DMA
    args = (
        atoms, edge_mask, norm_gain.reshape(1, D), w_query, w_key, w_value, w_out,
        bn_gain.reshape(1, D), bn_shift.reshape(1, D), w_up, w_down,
    )
    vm = pltpu.VMEM
    return pl.pallas_call(
        kernel,
        out_shape=jax.ShapeDtypeStruct((T, D), BF16),
        in_specs=[pl.BlockSpec(memory_space=pl.ANY)] * len(args),
        out_specs=pl.BlockSpec(memory_space=pl.ANY),
        scratch_shapes=[
            vm((T, D), BF16), vm((SLABS, T, T), jnp.int32), vm((1, D), F32),
            vm((D, D), BF16), vm((D, D), BF16), vm((D, D), BF16), vm((D, D), BF16),
            vm((1, D), F32), vm((1, D), F32), vm((D, FF), BF16), vm((FF, D), BF16),
            vm((T, D), BF16), vm((4, T, D), BF16), vm((D, D), BF16), vm((D, D), BF16),
            vm((HEADS, 2 * HEAD_DIM, T), BF16), vm((SLABS, HEADS // 2, T, 128), BF16),
            vm((SLABS, HEADS, VROWS, T), BF16), vm((SLABS, T, T), F32),
            vm((T, T), F32), vm((T, T), F32), vm((T, T), BF16), vm((T, T), BF16),
            vm((8, T), F32), vm((8, T), F32), vm((HEADS, 8, T), F32), vm((HEADS, AROWS, T), F32),
            vm((D, T), BF16), vm((T, D), F32), vm((T, D), BF16),
            vm((2, D), F32), vm((PLANE, 2, D), F32), vm((2, D), F32), vm((NZ, 2, D), F32),
            dma((15,)), dma((2,)), dma, dma, dma((CHUNKS,)), dma((CHUNKS,)),
            dma((CHUNKS,)), dma((CHUNKS,)), dma((CHUNKS,)), dma((CHUNKS,)),
            dma((PLANE,)), dma((PLANE,)), dma((NZ,)), dma((NZ,)),
        ],
        compiler_params=pltpu.CompilerParams(
            collective_id=0, has_side_effects=True, vmem_limit_bytes=63000 * 1024
        ),
    )(*args)


def solution(mesh):
    rows = P(("grp", "blk"), None)
    return jax.shard_map(
        body,
        mesh=mesh,
        in_specs=(rows, P(("grp", "blk"), None, None, None)) + (P(),) * 9,
        out_specs=rows,
        check_vma=False,
    )
```

```python
import functools
import math

import jax
import jax.numpy as jnp
from jax import lax
from jax.experimental import pallas as pl
from jax.experimental.pallas import tpu as pltpu
from jax.sharding import PartitionSpec as P

F32 = jnp.float32
BF16 = jnp.bfloat16
T = 512
D = 512
HEADS = 8
HEAD_DIM = 64
FF = 1024
SLABS = 5
VROWS = 80
AROWS = 72
CHUNKS = 2
CROWS = T // CHUNKS
NEG = -1e30
SCALE = HEAD_DIM**-0.5 * math.log2(math.e)
NY, NZ, NX = 4, 8, 2
PLANE = NX * NY * 2
BLOCKS = PLANE * NZ


def mm(a, b):
    return jnp.dot(a, b, preferred_element_type=F32)


def mm_nt(a, b):
    return lax.dot_general(a, b, (((1,), (1,)), ((), ())), preferred_element_type=F32)


def kernel(
    atoms_hbm, mask_hbm, gain_hbm, wq_hbm, wk_hbm, wv_hbm, wo_hbm, bng_hbm, bns_hbm, wu_hbm, wd_hbm,
    out_hbm,
    atoms, mask, gain, wq, wk, wv, wo, bng, bns, wu, wd,
    nrm, recv, wqt, wvt, qz, keys, vals, bias, t0, t1, a0, a1, top, acc,
    mixed, after, result, stat, stat_a, stat_m, stat_b,
    load_sem, out_sem, own_send, own_recv, fst_send, fst_recv, fwd_send, fwd_recv, snd_send, snd_recv,
    sa_send, sa_recv, sb_send, sb_recv,
):
    me = lax.axis_index("blk")
    core = lax.rem(me, 2)
    y = lax.rem(me // 2, NY)
    z = lax.rem(me // (2 * NY), NZ)
    xh = me // (2 * NY * NZ)
    sgn = 1 - 2 * core
    partner = me + sgn
    ahead = lax.rem(me + 2 * sgn + BLOCKS, BLOCKS)
    behind = lax.rem(me - 2 * sgn + BLOCKS, BLOCKS)
    place = xh * (NY * 2) + y * 2 + core

    def plane_peer(j):
        u = lax.rem(place + j, PLANE)
        return ((u // (NY * 2)) * NZ + z) * (NY * 2) + lax.rem(u, NY * 2)

    def line_peer(j):
        return (xh * NZ + lax.rem(z + j, NZ)) * (NY * 2) + y * 2 + core

    offsets = [2, 2 + sgn, 2 + 2 * sgn, 2 - sgn, 2 - 2 * sgn]
    loads = [
        pltpu.make_async_copy(atoms_hbm, atoms, load_sem.at[0]),
        pltpu.make_async_copy(gain_hbm, gain, load_sem.at[1]),
        pltpu.make_async_copy(wq_hbm, wq, load_sem.at[2]),
        pltpu.make_async_copy(wk_hbm, wk, load_sem.at[3]),
        pltpu.make_async_copy(wv_hbm, wv, load_sem.at[4]),
    ]
    mask_loads = [
        pltpu.make_async_copy(mask_hbm.at[0, offsets[s]], mask.at[s], load_sem.at[5 + s])
        for s in range(SLABS)
    ]
    late = [
        pltpu.make_async_copy(wo_hbm, wo, load_sem.at[10]),
        pltpu.make_async_copy(bng_hbm, bng, load_sem.at[11]),
        pltpu.make_async_copy(bns_hbm, bns, load_sem.at[12]),
        pltpu.make_async_copy(wu_hbm, wu, load_sem.at[13]),
        pltpu.make_async_copy(wd_hbm, wd, load_sem.at[14]),
    ]
    for copy in loads + mask_loads + late:
        copy.start()

    barrier = pltpu.get_barrier_semaphore()
    peers = [partner, ahead, behind]
    peers += [plane_peer(j) for j in range(1, PLANE)]
    peers += [line_peer(j) for j in range(1, NZ)]
    for peer in peers:
        pl.semaphore_signal(
            barrier, inc=1, device_id={"blk": peer}, device_id_type=pl.DeviceIdType.MESH
        )

    def remote(src, dst, send, rec, device):
        return pltpu.make_async_remote_copy(
            src_ref=src, dst_ref=dst, send_sem=send, recv_sem=rec,
            device_id={"blk": device}, device_id_type=pl.DeviceIdType.MESH,
        )

    def rows(c):
        return pl.ds(c * CROWS, CROWS)

    own = remote(nrm, recv.at[0], own_send, own_recv, partner)
    first = [
        remote(nrm.at[rows(c)], recv.at[1, rows(c)], fst_send.at[c], fst_recv.at[c], behind)
        for c in range(CHUNKS)
    ]
    passed = [
        remote(recv.at[1, rows(c)], recv.at[2, rows(c)], fwd_send.at[c], fwd_recv.at[c], partner)
        for c in range(CHUNKS)
    ]
    second = [
        remote(nrm.at[rows(c)], recv.at[3, rows(c)], snd_send.at[c], snd_recv.at[c], ahead)
        for c in range(CHUNKS)
    ]

    with jax.named_scope("w_atoms"):
        loads[0].wait()
        loads[1].wait()
    x = atoms[...].astype(F32)
    nrm[...] = (
        x * lax.rsqrt(jnp.mean(x * x, axis=-1, keepdims=True) + 1e-6) * gain[...]
    ).astype(BF16)
    with jax.named_scope("w_barrier"):
        pl.semaphore_wait(barrier, len(peers))
    for copy in first:
        copy.start()
    own.start()

    with jax.named_scope("w_weights"):
        for copy in loads[2:]:
            copy.wait()
    wqt[...] = wq[...].T
    wvt[...] = wv[...].T

    def project(slot, features):
        k = mm(features, wk[...]).astype(BF16)
        for pair in range(HEADS // 2):
            keys[slot, pair] = k[:, pair * 128 : (pair + 1) * 128]
        v = mm_nt(wvt[...], features).astype(BF16)
        for h in range(HEADS):
            vals[slot, h, 0:HEAD_DIM] = v[h * HEAD_DIM : (h + 1) * HEAD_DIM]

    def make_bias(slot):
        mask_loads[slot].wait()
        for kc in range(T // 128):
            allowed = mask[slot, :, kc * 128 : (kc + 1) * 128] > 0
            if slot == 0:
                r = lax.broadcasted_iota(jnp.int32, (T, 128), 0)
                c = lax.broadcasted_iota(jnp.int32, (T, 128), 1) + kc * 128
                allowed = allowed | (r == c)
            bias[slot, kc * 128 : (kc + 1) * 128] = jnp.where(allowed, 0.0, NEG).astype(F32).T

    features = nrm[...]
    q = mm_nt(wqt[...], features).astype(BF16).astype(F32) * SCALE
    high = q.astype(BF16)
    low = (q - high.astype(F32)).astype(BF16)
    zero = jnp.zeros((HEAD_DIM, T), BF16)
    for h in range(HEADS):
        for i, piece in enumerate((high, low)):
            part = piece[h * HEAD_DIM : (h + 1) * HEAD_DIM]
            at = i * 2 * HEAD_DIM
            qz[h, at : at + HEAD_DIM] = part if h % 2 == 0 else zero
            qz[h, at + HEAD_DIM : at + 2 * HEAD_DIM] = zero if h % 2 == 0 else part
    for s in range(SLABS):
        for h in range(HEADS):
            vals[s, h, HEAD_DIM:VROWS] = jnp.ones((VROWS - HEAD_DIM, T), BF16)
    project(0, features)
    make_bias(0)

    def score(slot, h, fresh):
        t, a = (t0, a0) if h % 2 == 0 else (t1, a1)
        best = None
        for kc in range(2):
            ks = slice(kc * 256, (kc + 1) * 256)
            kp = keys[slot, h // 2, ks]
            s = mm(jnp.concatenate([kp, kp], axis=1), qz[h]) + bias[slot, ks]
            t[ks] = s
            m = jnp.max(s, axis=0, keepdims=True)
            best = m if best is None else jnp.maximum(best, m)
        if fresh:
            top[h] = jnp.broadcast_to(best, (8, T))
        else:
            old = top[h]
            new = jnp.maximum(old, best)
            a[...] = jnp.exp2(old - new)
            top[h] = new

    def gather(slot, h, fresh):
        t, a = (t0, a0) if h % 2 == 0 else (t1, a1)
        for qc in range(2):
            qs = slice(qc * 256, (qc + 1) * 256)
            m = top[h, 0:1, qs]
            p = jnp.exp2(t[:, qs] - m).astype(BF16)
            new = mm(vals[slot, h], p)[0:AROWS]
            if fresh:
                acc[h, :, qs] = new
            else:
                acc[h, :, qs] = acc[h, :, qs] * a[0:1, qs] + new

    def attend(slot, fresh=False):
        score(slot, 0, fresh)
        for h in range(HEADS):
            if h + 1 < HEADS:
                score(slot, h + 1, fresh)
            gather(slot, h, fresh)

    with jax.named_scope("w_partner"):
        own.wait_recv()
    with jax.named_scope("attend0"):
        project(1, recv[0])
        attend(0, fresh=True)
        make_bias(1)
    for copy in second:
        copy.start()
    with jax.named_scope("attend1"):
        attend(1)
    with jax.named_scope("w_first0"):
        first[0].wait_recv()
    passed[0].start()
    for s in range(2, SLABS):
        make_bias(s)
    with jax.named_scope("w_first1"):
        for copy in first[1:]:
            copy.wait_recv()
    for copy in passed[1:]:
        copy.start()
    with jax.named_scope("attend2"):
        project(2, recv[1])
        attend(2)
    with jax.named_scope("w_passed"):
        for copy in passed:
            copy.wait_recv()
    with jax.named_scope("attend3"):
        project(3, recv[2])
        attend(3)
    with jax.named_scope("w_second"):
        for copy in second:
            copy.wait_recv()
    with jax.named_scope("attend4"):
        project(4, recv[3])
        attend(4)

    for h in range(HEADS):
        a = acc[h]
        mixed[h * HEAD_DIM : (h + 1) * HEAD_DIM] = (
            a[0:HEAD_DIM] * (1.0 / a[HEAD_DIM : HEAD_DIM + 1])
        ).astype(BF16)
    for copy in late:
        copy.wait()
    mix = mixed[...].T
    res = atoms[...].astype(F32) + mm(mix, wo[...])
    after[...] = res

    mean = jnp.sum(res, axis=0, keepdims=True) * (1.0 / T)
    dev = after[...] - mean
    m2 = jnp.sum(dev * dev, axis=0, keepdims=True)
    stat[0:1] = mean
    stat[1:2] = m2

    def merge(mean, m2, others, count, size):
        total = mean
        for j in range(1, count):
            total = total + others[j, 0:1]
        new = total * (1.0 / count)
        spread = (mean - new) * (mean - new)
        for j in range(1, count):
            d = others[j, 0:1] - new
            spread = spread + d * d
            m2 = m2 + others[j, 1:2]
        return new, m2 + spread * size

    plane = [
        remote(stat, stat_a.at[j], sa_send.at[j], sa_recv.at[j], plane_peer(j))
        for j in range(1, PLANE)
    ]
    for copy in plane:
        copy.start()
    with jax.named_scope("w_plane"):
        for copy in plane:
            copy.wait_recv()
    mean, m2 = merge(mean, m2, stat_a, PLANE, float(T))
    stat_m[0:1] = mean
    stat_m[1:2] = m2
    line = [
        remote(stat_m, stat_b.at[j], sb_send.at[j], sb_recv.at[j], line_peer(j))
        for j in range(1, NZ)
    ]
    for copy in line:
        copy.start()
    with jax.named_scope("w_line"):
        for copy in line:
            copy.wait_recv()
    mean, m2 = merge(mean, m2, stat_b, NZ, float(T * PLANE))
    var = m2 * (1.0 / (T * BLOCKS))
    factor = lax.rsqrt(var + 1e-5) * bng[...]

    outs = []
    for c in range(2):
        rs = slice(c * 256, (c + 1) * 256)
        a = after[rs]
        batched = ((a - mean) * factor + bns[...]).astype(BF16)
        hidden = jax.nn.gelu(mm(batched, wu[...]), approximate=True).astype(BF16)
        result[rs] = (a + mm(hidden, wd[...])).astype(BF16)
        copy = pltpu.make_async_copy(result.at[rs], out_hbm.at[rs], out_sem.at[c])
        copy.start()
        outs.append(copy)

    own.wait_send()
    for copy in first + passed + second + plane + line:
        copy.wait_send()
    with jax.named_scope("w_outs"):
        for copy in outs:
            copy.wait()


def body(atoms, edge_mask, norm_gain, w_query, w_key, w_value, w_out, bn_gain, bn_shift, w_up, w_down):
    dma = pltpu.SemaphoreType.DMA
    args = (
        atoms, edge_mask, norm_gain.reshape(1, D), w_query, w_key, w_value, w_out,
        bn_gain.reshape(1, D), bn_shift.reshape(1, D), w_up, w_down,
    )
    vm = pltpu.VMEM
    return pl.pallas_call(
        kernel,
        out_shape=jax.ShapeDtypeStruct((T, D), BF16),
        in_specs=[pl.BlockSpec(memory_space=pl.ANY)] * len(args),
        out_specs=pl.BlockSpec(memory_space=pl.ANY),
        scratch_shapes=[
            vm((T, D), BF16), vm((SLABS, T, T), jnp.int32), vm((1, D), F32),
            vm((D, D), BF16), vm((D, D), BF16), vm((D, D), BF16), vm((D, D), BF16),
            vm((1, D), F32), vm((1, D), F32), vm((D, FF), BF16), vm((FF, D), BF16),
            vm((T, D), BF16), vm((4, T, D), BF16), vm((D, D), BF16), vm((D, D), BF16),
            vm((HEADS, 4 * HEAD_DIM, T), BF16), vm((SLABS, HEADS // 2, T, 128), BF16),
            vm((SLABS, HEADS, VROWS, T), BF16), vm((SLABS, T, T), F32),
            vm((T, T), F32), vm((T, T), F32),
            vm((8, T), F32), vm((8, T), F32), vm((HEADS, 8, T), F32), vm((HEADS, AROWS, T), F32),
            vm((D, T), BF16), vm((T, D), F32), vm((T, D), BF16),
            vm((2, D), F32), vm((PLANE, 2, D), F32), vm((2, D), F32), vm((NZ, 2, D), F32),
            dma((15,)), dma((2,)), dma, dma, dma((CHUNKS,)), dma((CHUNKS,)),
            dma((CHUNKS,)), dma((CHUNKS,)), dma((CHUNKS,)), dma((CHUNKS,)),
            dma((PLANE,)), dma((PLANE,)), dma((NZ,)), dma((NZ,)),
        ],
        compiler_params=pltpu.CompilerParams(
            collective_id=0, has_side_effects=True, vmem_limit_bytes=63000 * 1024
        ),
    )(*args)


def solution(mesh):
    rows = P(("grp", "blk"), None)
    return jax.shard_map(
        body,
        mesh=mesh,
        in_specs=(rows, P(("grp", "blk"), None, None, None)) + (P(),) * 9,
        out_specs=rows,
        check_vma=False,
    )
```

```python
import functools
import math

import jax
import jax.numpy as jnp
from jax import lax
from jax.experimental import pallas as pl
from jax.experimental.pallas import tpu as pltpu
from jax.sharding import PartitionSpec as P

F32 = jnp.float32
BF16 = jnp.bfloat16
T = 512
D = 512
HEADS = 8
HEAD_DIM = 64
FF = 1024
SLABS = 5
VROWS = 80
AROWS = 72
CHUNKS = 2
CROWS = T // CHUNKS
NEG = -1e30
SCALE = HEAD_DIM**-0.5 * math.log2(math.e)
NY, NZ, NX = 4, 8, 2
PLANE = NX * NY * 2
BLOCKS = PLANE * NZ


def mm(a, b):
    return jnp.dot(a, b, preferred_element_type=F32)


def mm_nt(a, b):
    return lax.dot_general(a, b, (((1,), (1,)), ((), ())), preferred_element_type=F32)


def kernel(
    atoms, mask_hbm, gain, wq_hbm, wk_hbm, wv_hbm, wo_hbm, bng, bns, wu_hbm, wd_hbm,
    out,
    mask, wq, wk, wv, wo, wu, wd,
    nrm, recv, wqt, wvt, qz, keys, vals, bias, t0, t1, a0, a1, top, acc,
    mixed, after, stat, stat_a, stat_m, stat_b,
    load_sem, own_send, own_recv, fst_send, fst_recv, fwd_send, fwd_recv, snd_send, snd_recv,
    sa_send, sa_recv, sb_send, sb_recv,
):
    me = lax.axis_index("blk")
    core = lax.rem(me, 2)
    y = lax.rem(me // 2, NY)
    z = lax.rem(me // (2 * NY), NZ)
    xh = me // (2 * NY * NZ)
    sgn = 1 - 2 * core
    partner = me + sgn
    ahead = lax.rem(me + 2 * sgn + BLOCKS, BLOCKS)
    behind = lax.rem(me - 2 * sgn + BLOCKS, BLOCKS)
    place = xh * (NY * 2) + y * 2 + core

    def plane_peer(j):
        u = lax.rem(place + j, PLANE)
        return ((u // (NY * 2)) * NZ + z) * (NY * 2) + lax.rem(u, NY * 2)

    def line_peer(j):
        return (xh * NZ + lax.rem(z + j, NZ)) * (NY * 2) + y * 2 + core

    offsets = [2, 2 + sgn, 2 + 2 * sgn, 2 - sgn, 2 - 2 * sgn]
    loads = [
        pltpu.make_async_copy(wq_hbm, wq, load_sem.at[0]),
        pltpu.make_async_copy(wk_hbm, wk, load_sem.at[1]),
        pltpu.make_async_copy(wv_hbm, wv, load_sem.at[2]),
    ]
    mask_loads = [
        pltpu.make_async_copy(mask_hbm.at[0, offsets[s]], mask.at[s], load_sem.at[3 + s])
        for s in range(SLABS)
    ]
    late = [
        pltpu.make_async_copy(wo_hbm, wo, load_sem.at[8]),
        pltpu.make_async_copy(wu_hbm, wu, load_sem.at[9]),
        pltpu.make_async_copy(wd_hbm, wd, load_sem.at[10]),
    ]
    for copy in loads + mask_loads + late:
        copy.start()

    barrier = pltpu.get_barrier_semaphore()
    peers = [partner, ahead, behind]
    peers += [plane_peer(j) for j in range(1, PLANE)]
    peers += [line_peer(j) for j in range(1, NZ)]
    for peer in peers:
        pl.semaphore_signal(
            barrier, inc=1, device_id={"blk": peer}, device_id_type=pl.DeviceIdType.MESH
        )

    def remote(src, dst, send, rec, device):
        return pltpu.make_async_remote_copy(
            src_ref=src, dst_ref=dst, send_sem=send, recv_sem=rec,
            device_id={"blk": device}, device_id_type=pl.DeviceIdType.MESH,
        )

    def rows(c):
        return pl.ds(c * CROWS, CROWS)

    own_keys = remote(keys.at[0], keys.at[1], own_send.at[0], own_recv.at[0], partner)
    own_vals = remote(vals.at[0], vals.at[1], own_send.at[1], own_recv.at[1], partner)
    first = [
        remote(nrm.at[rows(c)], recv.at[0, rows(c)], fst_send.at[c], fst_recv.at[c], behind)
        for c in range(CHUNKS)
    ]
    passed = [
        remote(recv.at[0, rows(c)], recv.at[1, rows(c)], fwd_send.at[c], fwd_recv.at[c], partner)
        for c in range(CHUNKS)
    ]
    second = [
        remote(nrm.at[rows(c)], recv.at[2, rows(c)], snd_send.at[c], snd_recv.at[c], ahead)
        for c in range(CHUNKS)
    ]

    x = atoms[...].astype(F32)
    nrm[...] = (
        x * lax.rsqrt(jnp.mean(x * x, axis=-1, keepdims=True) + 1e-6) * gain[...]
    ).astype(BF16)
    with jax.named_scope("w_barrier"):
        pl.semaphore_wait(barrier, len(peers))
    for copy in first:
        copy.start()

    with jax.named_scope("w_weights"):
        for copy in loads:
            copy.wait()
    wqt[...] = wq[...].T
    wvt[...] = wv[...].T

    def project(slot, features):
        k = mm(features, wk[...]).astype(BF16)
        for pair in range(HEADS // 2):
            keys[slot, pair] = k[:, pair * 128 : (pair + 1) * 128]
        v = mm_nt(wvt[...], features).astype(BF16)
        for h in range(HEADS):
            vals[slot, h, 0:HEAD_DIM] = v[h * HEAD_DIM : (h + 1) * HEAD_DIM]

    def make_bias(slot):
        mask_loads[slot].wait()
        for kc in range(T // 128):
            allowed = mask[slot, :, kc * 128 : (kc + 1) * 128] > 0
            if slot == 0:
                r = lax.broadcasted_iota(jnp.int32, (T, 128), 0)
                c = lax.broadcasted_iota(jnp.int32, (T, 128), 1) + kc * 128
                allowed = allowed | (r == c)
            bias[slot, kc * 128 : (kc + 1) * 128] = jnp.where(allowed, 0.0, NEG).astype(F32).T

    features = nrm[...]
    q = mm_nt(wqt[...], features).astype(BF16).astype(F32) * SCALE
    high = q.astype(BF16)
    low = (q - high.astype(F32)).astype(BF16)
    zero = jnp.zeros((HEAD_DIM, T), BF16)
    for h in range(HEADS):
        for i, piece in enumerate((high, low)):
            part = piece[h * HEAD_DIM : (h + 1) * HEAD_DIM]
            at = i * 2 * HEAD_DIM
            qz[h, at : at + HEAD_DIM] = part if h % 2 == 0 else zero
            qz[h, at + HEAD_DIM : at + 2 * HEAD_DIM] = zero if h % 2 == 0 else part
    for s in (0, 2, 3, 4):
        for h in range(HEADS):
            vals[s, h, HEAD_DIM:VROWS] = jnp.ones((VROWS - HEAD_DIM, T), BF16)
    project(0, features)
    own_keys.start()
    own_vals.start()
    with jax.named_scope("biases"):
        for s in range(SLABS):
            make_bias(s)

    halves = (slice(0, 256), slice(256, 512))

    def score(slot, h, fresh):
        t, a = (t0, a0) if h % 2 == 0 else (t1, a1)
        for qs in halves:
            best = None
            for ks in halves:
                kp = keys[slot, h // 2, ks]
                s = mm(jnp.concatenate([kp, kp], axis=1), qz[h, :, qs]) + bias[slot, ks, qs]
                t[ks, qs] = s
                m = jnp.max(s.reshape(32, 8, 256), axis=0)
                best = m if best is None else jnp.maximum(best, m)
            best = jnp.max(best, axis=0, keepdims=True)
            if fresh:
                top[h, :, qs] = jnp.broadcast_to(best, (8, 256))
            else:
                old = top[h, :, qs]
                new = jnp.maximum(old, best)
                a[:, qs] = jnp.exp2(old - new)
                top[h, :, qs] = new

    def gather(slot, h, fresh):
        t, a = (t0, a0) if h % 2 == 0 else (t1, a1)
        for qs in halves:
            p = jnp.exp2(t[:, qs] - top[h, 0:1, qs]).astype(BF16)
            new = mm(vals[slot, h], p)[0:AROWS]
            if fresh:
                acc[h, :, qs] = new
            else:
                acc[h, :, qs] = acc[h, :, qs] * a[0:1, qs] + new

    def attend(slots):
        steps = [(slot, h, slot == 0) for slot in slots for h in range(HEADS)]
        score(*steps[0])
        for i, step in enumerate(steps):
            if i + 1 < len(steps):
                score(*steps[i + 1])
            gather(*step)

    with jax.named_scope("attend0"):
        attend([0])
    for copy in second:
        copy.start()
    with jax.named_scope("w_partner"):
        own_keys.wait_recv()
        own_vals.wait_recv()
    with jax.named_scope("attend1"):
        attend([1])
    with jax.named_scope("w_first"):
        for copy in first:
            copy.wait_recv()
    for copy in passed:
        copy.start()
    with jax.named_scope("attend2"):
        project(2, recv[0])
        attend([2])
    with jax.named_scope("w_passed"):
        for copy in passed:
            copy.wait_recv()
    with jax.named_scope("attend3"):
        project(3, recv[1])
        attend([3])
    with jax.named_scope("w_second"):
        for copy in second:
            copy.wait_recv()
    with jax.named_scope("attend4"):
        project(4, recv[2])
        attend([4])

    for h in range(HEADS):
        a = acc[h]
        mixed[h * HEAD_DIM : (h + 1) * HEAD_DIM] = (
            a[0:HEAD_DIM] * (1.0 / a[HEAD_DIM : HEAD_DIM + 1])
        ).astype(BF16)
    for copy in late:
        copy.wait()
    mix = mixed[...].T
    res = atoms[...].astype(F32) + mm(mix, wo[...])
    after[...] = res

    mean = jnp.sum(res, axis=0, keepdims=True) * (1.0 / T)
    dev = after[...] - mean
    m2 = jnp.sum(dev * dev, axis=0, keepdims=True)
    stat[0:1] = mean
    stat[1:2] = m2

    def merge(mean, m2, others, count, size):
        total = mean
        for j in range(1, count):
            total = total + others[j, 0:1]
        new = total * (1.0 / count)
        spread = (mean - new) * (mean - new)
        for j in range(1, count):
            d = others[j, 0:1] - new
            spread = spread + d * d
            m2 = m2 + others[j, 1:2]
        return new, m2 + spread * size

    plane = [
        remote(stat, stat_a.at[j], sa_send.at[j], sa_recv.at[j], plane_peer(j))
        for j in range(1, PLANE)
    ]
    for copy in plane:
        copy.start()
    with jax.named_scope("w_plane"):
        for copy in plane:
            copy.wait_recv()
    mean, m2 = merge(mean, m2, stat_a, PLANE, float(T))
    stat_m[0:1] = mean
    stat_m[1:2] = m2
    line = [
        remote(stat_m, stat_b.at[j], sb_send.at[j], sb_recv.at[j], line_peer(j))
        for j in range(1, NZ)
    ]
    for copy in line:
        copy.start()
    with jax.named_scope("w_line"):
        for copy in line:
            copy.wait_recv()
    mean, m2 = merge(mean, m2, stat_b, NZ, float(T * PLANE))
    var = m2 * (1.0 / (T * BLOCKS))
    factor = lax.rsqrt(var + 1e-5) * bng[...]

    for c in range(2):
        rs = slice(c * 256, (c + 1) * 256)
        a = after[rs]
        batched = ((a - mean) * factor + bns[...]).astype(BF16)
        hidden = jax.nn.gelu(mm(batched, wu[...]), approximate=True).astype(BF16)
        out[rs] = (a + mm(hidden, wd[...])).astype(BF16)

    own_keys.wait_send()
    own_vals.wait_send()
    for copy in first + passed + second + plane + line:
        copy.wait_send()


def body(atoms, edge_mask, norm_gain, w_query, w_key, w_value, w_out, bn_gain, bn_shift, w_up, w_down):
    dma = pltpu.SemaphoreType.DMA
    args = (
        atoms, edge_mask, norm_gain.reshape(1, D), w_query, w_key, w_value, w_out,
        bn_gain.reshape(1, D), bn_shift.reshape(1, D), w_up, w_down,
    )
    vm = pltpu.VMEM
    return pl.pallas_call(
        kernel,
        out_shape=jax.ShapeDtypeStruct((T, D), BF16),
        in_specs=[pl.BlockSpec(memory_space=vm if i in (0, 2, 7, 8) else pl.ANY) for i in range(len(args))],
        out_specs=pl.BlockSpec(memory_space=pltpu.VMEM),
        scratch_shapes=[
            vm((SLABS, T, T), jnp.int32),
            vm((D, D), BF16), vm((D, D), BF16), vm((D, D), BF16), vm((D, D), BF16),
            vm((D, FF), BF16), vm((FF, D), BF16),
            vm((T, D), BF16), vm((3, T, D), BF16), vm((D, D), BF16), vm((D, D), BF16),
            vm((HEADS, 4 * HEAD_DIM, T), BF16), vm((SLABS, HEADS // 2, T, 128), BF16),
            vm((SLABS, HEADS, VROWS, T), BF16), vm((SLABS, T, T), F32),
            vm((T, T), F32), vm((T, T), F32),
            vm((8, T), F32), vm((8, T), F32), vm((HEADS, 8, T), F32), vm((HEADS, AROWS, T), F32),
            vm((D, T), BF16), vm((T, D), F32),
            vm((2, D), F32), vm((PLANE, 2, D), F32), vm((2, D), F32), vm((NZ, 2, D), F32),
            dma((11,)), dma((2,)), dma((2,)), dma((CHUNKS,)), dma((CHUNKS,)),
            dma((CHUNKS,)), dma((CHUNKS,)), dma((CHUNKS,)), dma((CHUNKS,)),
            dma((PLANE,)), dma((PLANE,)), dma((NZ,)), dma((NZ,)),
        ],
        compiler_params=pltpu.CompilerParams(
            collective_id=0, has_side_effects=True, vmem_limit_bytes=54000 * 1024
        ),
    )(*args)


def solution(mesh):
    rows = P(("grp", "blk"), None)
    return jax.shard_map(
        body,
        mesh=mesh,
        in_specs=(rows, P(("grp", "blk"), None, None, None)) + (P(),) * 9,
        out_specs=rows,
        check_vma=False,
    )
```

```python
import functools
import math

import jax
import jax.numpy as jnp
from jax import lax
from jax.experimental import pallas as pl
from jax.experimental.pallas import tpu as pltpu
from jax.sharding import PartitionSpec as P

F32 = jnp.float32
BF16 = jnp.bfloat16
T = 512
D = 512
HEADS = 8
HEAD_DIM = 64
FF = 1024
SLABS = 5
OWN = 0
VROWS = 80
AROWS = 72
CHUNKS = 2
CROWS = T // CHUNKS
NEG = -1e30
SCALE = HEAD_DIM**-0.5 * math.log2(math.e)
NY, NZ, NX = 4, 8, 2
PLANE = NX * NY * 2
BLOCKS = PLANE * NZ


def mm(a, b):
    return jnp.dot(a, b, preferred_element_type=F32)


def mm_nt(a, b):
    return lax.dot_general(a, b, (((1,), (1,)), ((), ())), preferred_element_type=F32)


def kernel(
    atoms_hbm, mask_hbm, gain_hbm, wq_hbm, wk_hbm, wv_hbm, wo_hbm, bng_hbm, bns_hbm, wu_hbm, wd_hbm,
    out_hbm,
    atoms, mask, gain, wq, wk, wv, wo, bng, bns, wu, wd,
    nrm, recv, wqt, wvt, qz, keys, vals, bias, t0, t1, a0, a1, top, acc,
    mixed, after, result, stat, stat_a, stat_m, stat_b,
    load_sem, out_sem, own_send, own_recv, fst_send, fwd_send, snd_send, arrive,
    sa_send, sa_recv, sb_send, sb_recv,
):
    me = lax.axis_index("blk")
    core = lax.rem(me, 2)
    y = lax.rem(me // 2, NY)
    z = lax.rem(me // (2 * NY), NZ)
    xh = me // (2 * NY * NZ)
    sgn = 1 - 2 * core
    partner = me + sgn
    ahead = lax.rem(me + 2 * sgn + BLOCKS, BLOCKS)
    behind = lax.rem(me - 2 * sgn + BLOCKS, BLOCKS)
    place = xh * (NY * 2) + y * 2 + core

    grp = lax.axis_index("grp")
    x = xh * 2 + grp

    def coords(index):
        return lax.rem(index // 2, NY), lax.rem(index // (2 * NY), NZ)

    def spot(dx, yz):
        there = lax.rem(x + dx + 2 * NX, 2 * NX)
        block = (((there // 2) * NZ + yz[1]) * NY + yz[0]) * 2 + core
        return {"grp": lax.rem(there, 2), "blk": block}

    far_behind = jnp.where(behind // (2 * NY * NZ) == xh, 0, 1)
    far_ahead = jnp.where(ahead // (2 * NY * NZ) == xh, 0, 1)
    relay = spot(-1, (y, z))

    def pick(far, blk):
        return {
            "grp": grp + far * (relay["grp"] - grp),
            "blk": blk + far * (relay["blk"] - blk),
        }

    def plane_peer(j):
        u = lax.rem(place + j, PLANE)
        return ((u // (NY * 2)) * NZ + z) * (NY * 2) + lax.rem(u, NY * 2)

    def line_peer(j):
        return (xh * NZ + lax.rem(z + j, NZ)) * (NY * 2) + y * 2 + core

    offsets = [2, 2 + sgn, 2 + 2 * sgn, 2 - sgn, 2 - 2 * sgn]
    loads = [
        pltpu.make_async_copy(atoms_hbm, atoms, load_sem.at[11]),
        pltpu.make_async_copy(gain_hbm, gain, load_sem.at[12]),
        pltpu.make_async_copy(wq_hbm, wq, load_sem.at[0]),
        pltpu.make_async_copy(wk_hbm, wk, load_sem.at[1]),
        pltpu.make_async_copy(wv_hbm, wv, load_sem.at[2]),
    ]
    mask_loads = [
        pltpu.make_async_copy(mask_hbm.at[0, offsets[s]], mask.at[s], load_sem.at[3 + s])
        for s in range(SLABS)
    ]
    late = [
        pltpu.make_async_copy(wo_hbm, wo, load_sem.at[8]),
        pltpu.make_async_copy(bng_hbm, bng, load_sem.at[13]),
        pltpu.make_async_copy(bns_hbm, bns, load_sem.at[14]),
        pltpu.make_async_copy(wu_hbm, wu, load_sem.at[9]),
        pltpu.make_async_copy(wd_hbm, wd, load_sem.at[10]),
    ]
    for copy in loads + mask_loads + late:
        copy.start()

    barrier = pltpu.get_barrier_semaphore()
    peers = [partner, ahead, behind]
    peers += [plane_peer(j) for j in range(1, PLANE)]
    peers += [line_peer(j) for j in range(1, NZ)]
    peers = [{"grp": grp, "blk": peer} for peer in peers]
    for place_yz in ((y, z), coords(behind), coords(ahead)):
        peers += [spot(-1, place_yz), spot(1, place_yz)]
    for peer in peers:
        pl.semaphore_signal(
            barrier, inc=1, device_id=peer, device_id_type=pl.DeviceIdType.MESH
        )

    def remote(src, dst, send, rec, device):
        return pltpu.make_async_remote_copy(
            src_ref=src, dst_ref=dst, send_sem=send, recv_sem=rec,
            device_id=device if isinstance(device, dict) else {"blk": device},
            device_id_type=pl.DeviceIdType.MESH,
        )

    def rows(c):
        return pl.ds(c * CROWS, CROWS)

    own_keys = remote(keys.at[0], keys.at[1], own_send.at[0], own_recv.at[0], partner)
    own_vals = remote(vals.at[0], vals.at[1], own_send.at[1], own_recv.at[1], partner)
    first = [
        remote(nrm.at[rows(0)], recv.at[0, rows(0)], fst_send.at[0], arrive.at[0, 0], behind),
        remote(
            nrm.at[rows(1)], recv.at[3 * far_behind, rows(1)], fst_send.at[1],
            arrive.at[3 * far_behind, 1], pick(far_behind, behind),
        ),
    ]
    first_on = remote(
        recv.at[3, rows(1)], recv.at[0, rows(1)], fst_send.at[2], arrive.at[0, 1],
        spot(-1, coords(behind)),
    )
    passed = [
        remote(recv.at[0, rows(c)], recv.at[1, rows(c)], fwd_send.at[c], arrive.at[1, c], partner)
        for c in range(CHUNKS)
    ]
    second = [
        remote(nrm.at[rows(0)], recv.at[2, rows(0)], snd_send.at[0], arrive.at[2, 0], ahead),
        remote(
            nrm.at[rows(1)], recv.at[2 + 2 * far_ahead, rows(1)], snd_send.at[1],
            arrive.at[2 + 2 * far_ahead, 1], pick(far_ahead, ahead),
        ),
    ]
    second_on = remote(
        recv.at[4, rows(1)], recv.at[2, rows(1)], snd_send.at[2], arrive.at[2, 1],
        spot(-1, coords(ahead)),
    )

    def arrived(slot, c):
        remote(recv.at[slot, rows(c)], recv.at[slot, rows(c)], fst_send.at[0], arrive.at[slot, c], partner).wait_recv()

    def start(copies):
        for copy in copies:
            copy.start()

    with jax.named_scope("w_atoms"):
        loads[0].wait()
        loads[1].wait()
    x = atoms[...].astype(F32)
    nrm[...] = (
        x * lax.rsqrt(jnp.mean(x * x, axis=-1, keepdims=True) + 1e-6) * gain[...]
    ).astype(BF16)
    with jax.named_scope("w_barrier"):
        pl.semaphore_wait(barrier, len(peers))
    start(first)

    @pl.when(far_ahead == 1)
    def _():
        start(second)


    with jax.named_scope("w_weights"):
        for copy in loads[2:]:
            copy.wait()
    wqt[...] = wq[...].T
    wvt[...] = wv[...].T

    def project(slot, features):
        k = mm(features, wk[...]).astype(BF16)
        for pair in range(HEADS // 2):
            keys[slot, pair] = k[:, pair * 128 : (pair + 1) * 128]
        v = mm_nt(wvt[...], features).astype(BF16)
        for h in range(HEADS):
            vals[slot, h, 0:HEAD_DIM] = v[h * HEAD_DIM : (h + 1) * HEAD_DIM]

    def make_bias(slot):
        mask_loads[slot].wait()
        for kc in range(T // 128):
            allowed = mask[slot, :, kc * 128 : (kc + 1) * 128] > 0
            if slot == 0:
                r = lax.broadcasted_iota(jnp.int32, (T, 128), 0)
                c = lax.broadcasted_iota(jnp.int32, (T, 128), 1) + kc * 128
                allowed = allowed | (r == c)
            bias[slot, kc * 128 : (kc + 1) * 128] = jnp.where(allowed, 0.0, NEG).astype(F32).T

    features = nrm[...]
    q = mm_nt(wqt[...], features).astype(BF16).astype(F32) * SCALE
    high = q.astype(BF16)
    low = (q - high.astype(F32)).astype(BF16)
    zero = jnp.zeros((HEAD_DIM, T), BF16)
    for h in range(HEADS):
        for i, piece in enumerate((high, low)):
            part = piece[h * HEAD_DIM : (h + 1) * HEAD_DIM]
            at = i * 2 * HEAD_DIM
            qz[h, at : at + HEAD_DIM] = part if h % 2 == 0 else zero
            qz[h, at + HEAD_DIM : at + 2 * HEAD_DIM] = zero if h % 2 == 0 else part
    for s in (0, 2, 3, 4):
        for h in range(HEADS):
            vals[s, h, HEAD_DIM:VROWS] = jnp.ones((VROWS - HEAD_DIM, T), BF16)
    project(0, features)
    own_keys.start()
    own_vals.start()
    with jax.named_scope("biases"):
        for s in range(SLABS):
            make_bias(s)

    halves = (slice(0, 256), slice(256, 512))

    def score(slot, h, fresh):
        t, a = (t0, a0) if h % 2 == 0 else (t1, a1)
        for qs in halves:
            best = None
            for ks in halves:
                kp = keys[slot, h // 2, ks]
                s = mm(jnp.concatenate([kp, kp], axis=1), qz[h, :, qs]) + bias[slot, ks, qs]
                t[ks, qs] = s
                m = jnp.max(s.reshape(32, 8, 256), axis=0)
                best = m if best is None else jnp.maximum(best, m)
            best = jnp.max(best, axis=0, keepdims=True)
            if fresh:
                top[h, :, qs] = jnp.broadcast_to(best, (8, 256))
            else:
                old = top[h, :, qs]
                new = jnp.maximum(old, best)
                a[:, qs] = jnp.exp2(old - new)
                top[h, :, qs] = new

    def gather(slot, h, fresh):
        t, a = (t0, a0) if h % 2 == 0 else (t1, a1)
        for qs in halves:
            p = jnp.exp2(t[:, qs] - top[h, 0:1, qs]).astype(BF16)
            new = mm(vals[slot, h], p)[0:AROWS]
            if fresh:
                acc[h, :, qs] = new
            else:
                acc[h, :, qs] = acc[h, :, qs] * a[0:1, qs] + new

    def attend(slots):
        steps = [(slot, h, slot is OWN) for slot in slots for h in range(HEADS)]
        score(*steps[0])
        for i, step in enumerate(steps):
            if i + 1 < len(steps):
                score(*steps[i + 1])
            gather(*step)

    with jax.named_scope("attend0"):
        attend([OWN])

    @pl.when(far_ahead == 0)
    def _():
        start(second)

    @pl.when(far_behind == 1)
    def _():
        arrived(3, 1)
        first_on.start()

    with jax.named_scope("w_partner"):
        own_keys.wait_recv()
        own_vals.wait_recv()
    with jax.named_scope("attend1"):
        attend([1])

    @pl.when(far_ahead == 1)
    def _():
        arrived(4, 1)
        second_on.start()

    with jax.named_scope("w_first"):
        for c in range(CHUNKS):
            arrived(far_ahead, c)

    @pl.when(far_ahead == 0)
    def _():
        start(passed)

    with jax.named_scope("attend2"):
        project(2 + far_ahead, recv[far_ahead])
        attend([2 + far_ahead])
    with jax.named_scope("w_passed"):
        for c in range(CHUNKS):
            arrived(1 - far_ahead, c)

    @pl.when(far_ahead == 1)
    def _():
        start(passed)

    with jax.named_scope("attend3"):
        project(3 - far_ahead, recv[1 - far_ahead])
        attend([3 - far_ahead])
    with jax.named_scope("w_second"):
        for c in range(CHUNKS):
            arrived(2, c)
    with jax.named_scope("attend4"):
        project(4, recv[2])
        attend([4])

    for h in range(HEADS):
        a = acc[h]
        mixed[h * HEAD_DIM : (h + 1) * HEAD_DIM] = (
            a[0:HEAD_DIM] * (1.0 / a[HEAD_DIM : HEAD_DIM + 1])
        ).astype(BF16)
    for copy in late:
        copy.wait()
    mix = mixed[...].T
    res = atoms[...].astype(F32) + mm(mix, wo[...])
    after[...] = res

    mean = jnp.sum(res, axis=0, keepdims=True) * (1.0 / T)
    dev = after[...] - mean
    m2 = jnp.sum(dev * dev, axis=0, keepdims=True)
    stat[0:1] = mean
    stat[1:2] = m2

    def merge(mean, m2, others, count, size):
        total = mean
        for j in range(1, count):
            total = total + others[j, 0:1]
        new = total * (1.0 / count)
        spread = (mean - new) * (mean - new)
        for j in range(1, count):
            d = others[j, 0:1] - new
            spread = spread + d * d
            m2 = m2 + others[j, 1:2]
        return new, m2 + spread * size

    plane = [
        remote(stat, stat_a.at[j], sa_send.at[j], sa_recv.at[j], plane_peer(j))
        for j in range(1, PLANE)
    ]
    for copy in plane:
        copy.start()
    with jax.named_scope("w_plane"):
        for copy in plane:
            copy.wait_recv()
    mean, m2 = merge(mean, m2, stat_a, PLANE, float(T))
    stat_m[0:1] = mean
    stat_m[1:2] = m2
    line = [
        remote(stat_m, stat_b.at[j], sb_send.at[j], sb_recv.at[j], line_peer(j))
        for j in range(1, NZ)
    ]
    for copy in line:
        copy.start()
    with jax.named_scope("w_line"):
        for copy in line:
            copy.wait_recv()
    mean, m2 = merge(mean, m2, stat_b, NZ, float(T * PLANE))
    var = m2 * (1.0 / (T * BLOCKS))
    factor = lax.rsqrt(var + 1e-5) * bng[...]

    outs = []
    for c in range(2):
        rs = slice(c * 256, (c + 1) * 256)
        a = after[rs]
        batched = ((a - mean) * factor + bns[...]).astype(BF16)
        hidden = jax.nn.gelu(mm(batched, wu[...]), approximate=True).astype(BF16)
        result[rs] = (a + mm(hidden, wd[...])).astype(BF16)
        copy = pltpu.make_async_copy(result.at[rs], out_hbm.at[rs], out_sem.at[c])
        copy.start()
        outs.append(copy)

    own_keys.wait_send()
    own_vals.wait_send()

    @pl.when(far_behind == 1)
    def _():
        first_on.wait_send()

    @pl.when(far_ahead == 1)
    def _():
        second_on.wait_send()

    for copy in first + passed + second + plane + line:
        copy.wait_send()
    with jax.named_scope("w_outs"):
        for copy in outs:
            copy.wait()


def body(atoms, edge_mask, norm_gain, w_query, w_key, w_value, w_out, bn_gain, bn_shift, w_up, w_down):
    dma = pltpu.SemaphoreType.DMA
    args = (
        atoms, edge_mask, norm_gain.reshape(1, D), w_query, w_key, w_value, w_out,
        bn_gain.reshape(1, D), bn_shift.reshape(1, D), w_up, w_down,
    )
    vm = pltpu.VMEM
    return pl.pallas_call(
        kernel,
        out_shape=jax.ShapeDtypeStruct((T, D), BF16),
        in_specs=[pl.BlockSpec(memory_space=pl.ANY)] * len(args),
        out_specs=pl.BlockSpec(memory_space=pl.ANY),
        scratch_shapes=[
            vm((T, D), BF16), vm((SLABS, T, T), jnp.int32), vm((1, D), F32),
            vm((D, D), BF16), vm((D, D), BF16), vm((D, D), BF16), vm((D, D), BF16),
            vm((1, D), F32), vm((1, D), F32), vm((D, FF), BF16), vm((FF, D), BF16),
            vm((T, D), BF16), vm((5, T, D), BF16), vm((D, D), BF16), vm((D, D), BF16),
            vm((HEADS, 4 * HEAD_DIM, T), BF16), vm((SLABS, HEADS // 2, T, 128), BF16),
            vm((SLABS, HEADS, VROWS, T), BF16), vm((SLABS, T, T), F32),
            vm((T, T), F32), vm((T, T), F32),
            vm((8, T), F32), vm((8, T), F32), vm((HEADS, 8, T), F32), vm((HEADS, AROWS, T), F32),
            vm((D, T), BF16), vm((T, D), F32), vm((T, D), BF16),
            vm((2, D), F32), vm((PLANE, 2, D), F32), vm((2, D), F32), vm((NZ, 2, D), F32),
            dma((15,)), dma((2,)), dma((2,)), dma((2,)), dma((3,)), dma((CHUNKS,)), dma((3,)),
            dma((5, CHUNKS)), dma((PLANE,)), dma((PLANE,)), dma((NZ,)), dma((NZ,)),
        ],
        compiler_params=pltpu.CompilerParams(
            collective_id=0, has_side_effects=True, vmem_limit_bytes=63000 * 1024
        ),
    )(*args)


def solution(mesh):
    rows = P(("grp", "blk"), None)
    return jax.shard_map(
        body,
        mesh=mesh,
        in_specs=(rows, P(("grp", "blk"), None, None, None)) + (P(),) * 9,
        out_specs=rows,
        check_vma=False,
    )
```

```python
import functools
import math

import jax
import jax.numpy as jnp
from jax import lax
from jax.experimental import pallas as pl
from jax.experimental.pallas import tpu as pltpu
from jax.sharding import PartitionSpec as P

F32 = jnp.float32
BF16 = jnp.bfloat16
T = 512
D = 512
HEADS = 8
HEAD_DIM = 64
FF = 1024
SLABS = 5
OWN = 0
VROWS = 80
AROWS = 72
CHUNKS = 2
CROWS = T // CHUNKS
NEG = -1e30
SCALE = HEAD_DIM**-0.5 * math.log2(math.e)
NY, NZ, NX = 4, 8, 2
PLANE = NX * NY * 2
BLOCKS = PLANE * NZ


def mm(a, b):
    return jnp.dot(a, b, preferred_element_type=F32)


def mm_nt(a, b):
    return lax.dot_general(a, b, (((1,), (1,)), ((), ())), preferred_element_type=F32)


def kernel(
    atoms_hbm, mask_hbm, gain_hbm, wq_hbm, wk_hbm, wv_hbm, wo_hbm, bng_hbm, bns_hbm, wu_hbm, wd_hbm,
    out_hbm,
    atoms, mask, gain, wq, wk, wv, wo, bng, bns, wu, wd,
    nrm, recv, wqt, wvt, qz, keys, vals, bias, t0, t1, a0, a1, top, acc,
    mixed, after, result, stat, stat_a, stat_m, stat_b,
    load_sem, out_sem, own_send, own_recv, fst_send, fwd_send, snd_send, arrive,
    sa_send, sa_recv, sb_send, sb_recv,
):
    me = lax.axis_index("blk")
    core = lax.rem(me, 2)
    y = lax.rem(me // 2, NY)
    z = lax.rem(me // (2 * NY), NZ)
    xh = me // (2 * NY * NZ)
    sgn = 1 - 2 * core
    partner = me + sgn
    ahead = lax.rem(me + 2 * sgn + BLOCKS, BLOCKS)
    behind = lax.rem(me - 2 * sgn + BLOCKS, BLOCKS)
    place = xh * (NY * 2) + y * 2 + core

    far_ahead = jnp.where(ahead // (2 * NY * NZ) == xh, 0, 1)

    def plane_peer(j):
        u = lax.rem(place + j, PLANE)
        return ((u // (NY * 2)) * NZ + z) * (NY * 2) + lax.rem(u, NY * 2)

    def line_peer(j):
        return (xh * NZ + lax.rem(z + j, NZ)) * (NY * 2) + y * 2 + core

    offsets = [2, 2 + sgn, 2 + 2 * sgn, 2 - sgn, 2 - 2 * sgn]
    loads = [
        pltpu.make_async_copy(atoms_hbm, atoms, load_sem.at[11]),
        pltpu.make_async_copy(gain_hbm, gain, load_sem.at[12]),
        pltpu.make_async_copy(wq_hbm, wq, load_sem.at[0]),
        pltpu.make_async_copy(wk_hbm, wk, load_sem.at[1]),
        pltpu.make_async_copy(wv_hbm, wv, load_sem.at[2]),
    ]
    mask_loads = [
        pltpu.make_async_copy(mask_hbm.at[0, offsets[s]], mask.at[s], load_sem.at[3 + s])
        for s in range(SLABS)
    ]
    late = [
        pltpu.make_async_copy(wo_hbm, wo, load_sem.at[8]),
        pltpu.make_async_copy(bng_hbm, bng, load_sem.at[13]),
        pltpu.make_async_copy(bns_hbm, bns, load_sem.at[14]),
        pltpu.make_async_copy(wu_hbm, wu, load_sem.at[9]),
        pltpu.make_async_copy(wd_hbm, wd, load_sem.at[10]),
    ]
    for copy in loads + mask_loads + late:
        copy.start()

    barrier = pltpu.get_barrier_semaphore()
    peers = [partner, ahead, behind]
    peers += [plane_peer(j) for j in range(1, PLANE)]
    peers += [line_peer(j) for j in range(1, NZ)]
    for peer in peers:
        pl.semaphore_signal(
            barrier, inc=1, device_id={"blk": peer}, device_id_type=pl.DeviceIdType.MESH
        )

    def remote(src, dst, send, rec, device):
        return pltpu.make_async_remote_copy(
            src_ref=src, dst_ref=dst, send_sem=send, recv_sem=rec,
            device_id={"blk": device}, device_id_type=pl.DeviceIdType.MESH,
        )

    def rows(c):
        return pl.ds(c * CROWS, CROWS)

    own_keys = remote(keys.at[0], keys.at[1], own_send.at[0], own_recv.at[0], partner)
    own_vals = remote(vals.at[0], vals.at[1], own_send.at[1], own_recv.at[1], partner)
    first = [
        remote(nrm.at[rows(c)], recv.at[0, rows(c)], fst_send.at[c], arrive.at[0, c], behind)
        for c in range(CHUNKS)
    ]
    passed = [
        remote(recv.at[0, rows(c)], recv.at[1, rows(c)], fwd_send.at[c], arrive.at[1, c], partner)
        for c in range(CHUNKS)
    ]
    second = [
        remote(nrm.at[rows(c)], recv.at[2, rows(c)], snd_send.at[c], arrive.at[2, c], ahead)
        for c in range(CHUNKS)
    ]

    def arrived(slot, c):
        remote(recv.at[slot, rows(c)], recv.at[slot, rows(c)], fst_send.at[0], arrive.at[slot, c], partner).wait_recv()

    def start(copies):
        for copy in copies:
            copy.start()

    with jax.named_scope("w_atoms"):
        loads[0].wait()
        loads[1].wait()
    x = atoms[...].astype(F32)
    nrm[...] = (
        x * lax.rsqrt(jnp.mean(x * x, axis=-1, keepdims=True) + 1e-6) * gain[...]
    ).astype(BF16)
    with jax.named_scope("w_barrier"):
        pl.semaphore_wait(barrier, len(peers))
    start(first)

    with jax.named_scope("w_weights"):
        for copy in loads[2:]:
            copy.wait()
    wqt[...] = wq[...].T
    wvt[...] = wv[...].T

    def project(slot, features):
        k = mm(features, wk[...]).astype(BF16)
        for pair in range(HEADS // 2):
            keys[slot, pair] = k[:, pair * 128 : (pair + 1) * 128]
        v = mm_nt(wvt[...], features).astype(BF16)
        for h in range(HEADS):
            vals[slot, h, 0:HEAD_DIM] = v[h * HEAD_DIM : (h + 1) * HEAD_DIM]

    def make_bias(slot):
        mask_loads[slot].wait()
        for kc in range(T // 128):
            allowed = mask[slot, :, kc * 128 : (kc + 1) * 128] > 0
            if slot == 0:
                r = lax.broadcasted_iota(jnp.int32, (T, 128), 0)
                c = lax.broadcasted_iota(jnp.int32, (T, 128), 1) + kc * 128
                allowed = allowed | (r == c)
            bias[slot, kc * 128 : (kc + 1) * 128] = jnp.where(allowed, 0.0, NEG).astype(F32).T

    features = nrm[...]
    q = mm_nt(wqt[...], features).astype(BF16).astype(F32) * SCALE
    high = q.astype(BF16)
    low = (q - high.astype(F32)).astype(BF16)
    zero = jnp.zeros((HEAD_DIM, T), BF16)
    for h in range(HEADS):
        for i, piece in enumerate((high, low)):
            part = piece[h * HEAD_DIM : (h + 1) * HEAD_DIM]
            at = i * 2 * HEAD_DIM
            qz[h, at : at + HEAD_DIM] = part if h % 2 == 0 else zero
            qz[h, at + HEAD_DIM : at + 2 * HEAD_DIM] = zero if h % 2 == 0 else part
    for s in (0, 2, 3, 4):
        for h in range(HEADS):
            vals[s, h, HEAD_DIM:VROWS] = jnp.ones((VROWS - HEAD_DIM, T), BF16)
    project(0, features)
    own_keys.start()
    own_vals.start()
    with jax.named_scope("biases"):
        for s in range(SLABS):
            make_bias(s)

    halves = (slice(0, 256), slice(256, 512))

    def score(slot, h, fresh):
        t, a = (t0, a0) if h % 2 == 0 else (t1, a1)
        for qs in halves:
            best = None
            for ks in halves:
                kp = keys[slot, h // 2, ks]
                s = mm(jnp.concatenate([kp, kp], axis=1), qz[h, :, qs]) + bias[slot, ks, qs]
                t[ks, qs] = s
                m = jnp.max(s.reshape(32, 8, 256), axis=0)
                best = m if best is None else jnp.maximum(best, m)
            best = jnp.max(best, axis=0, keepdims=True)
            if fresh:
                top[h, :, qs] = jnp.broadcast_to(best, (8, 256))
            else:
                old = top[h, :, qs]
                new = jnp.maximum(old, best)
                a[:, qs] = jnp.exp2(old - new)
                top[h, :, qs] = new

    def gather(slot, h, fresh):
        t, a = (t0, a0) if h % 2 == 0 else (t1, a1)
        for qs in halves:
            p = jnp.exp2(t[:, qs] - top[h, 0:1, qs]).astype(BF16)
            new = mm(vals[slot, h], p)[0:AROWS]
            if fresh:
                acc[h, :, qs] = new
            else:
                acc[h, :, qs] = acc[h, :, qs] * a[0:1, qs] + new

    def attend(slots):
        steps = [(slot, h, slot is OWN) for slot in slots for h in range(HEADS)]
        score(*steps[0])
        for i, step in enumerate(steps):
            if i + 1 < len(steps):
                score(*steps[i + 1])
            gather(*step)

    def fence():
        @pl.when(me < 0)
        def _():
            stat[...] = jnp.zeros_like(stat)

    fence()
    with jax.named_scope("attend0"):
        attend([OWN])
    fence()
    start(second)
    with jax.named_scope("w_partner"):
        own_keys.wait_recv()
        own_vals.wait_recv()
    fence()
    with jax.named_scope("attend1"):
        attend([1])
    fence()

    with jax.named_scope("w_first"):
        for c in range(CHUNKS):
            arrived(far_ahead, c)

    @pl.when(far_ahead == 0)
    def _():
        start(passed)

    with jax.named_scope("project2"):
        project(2 + far_ahead, recv[far_ahead])
    fence()
    with jax.named_scope("attend2"):
        attend([2 + far_ahead])
    fence()
    with jax.named_scope("w_passed"):
        for c in range(CHUNKS):
            arrived(1 - far_ahead, c)

    @pl.when(far_ahead == 1)
    def _():
        start(passed)

    with jax.named_scope("project3"):
        project(3 - far_ahead, recv[1 - far_ahead])
    fence()
    with jax.named_scope("attend3"):
        attend([3 - far_ahead])
    fence()
    with jax.named_scope("w_second"):
        for c in range(CHUNKS):
            arrived(2, c)
    with jax.named_scope("project4"):
        project(4, recv[2])
    fence()
    with jax.named_scope("attend4"):
        attend([4])
    fence()

    for h in range(HEADS):
        a = acc[h]
        mixed[h * HEAD_DIM : (h + 1) * HEAD_DIM] = (
            a[0:HEAD_DIM] * (1.0 / a[HEAD_DIM : HEAD_DIM + 1])
        ).astype(BF16)
    for copy in late:
        copy.wait()
    mix = mixed[...].T
    res = atoms[...].astype(F32) + mm(mix, wo[...])
    after[...] = res

    mean = jnp.sum(res, axis=0, keepdims=True) * (1.0 / T)
    dev = after[...] - mean
    m2 = jnp.sum(dev * dev, axis=0, keepdims=True)
    stat[0:1] = mean
    stat[1:2] = m2

    def merge(mean, m2, others, count, size):
        total = mean
        for j in range(1, count):
            total = total + others[j, 0:1]
        new = total * (1.0 / count)
        spread = (mean - new) * (mean - new)
        for j in range(1, count):
            d = others[j, 0:1] - new
            spread = spread + d * d
            m2 = m2 + others[j, 1:2]
        return new, m2 + spread * size

    plane = [
        remote(stat, stat_a.at[j], sa_send.at[j], sa_recv.at[j], plane_peer(j))
        for j in range(1, PLANE)
    ]
    for copy in plane:
        copy.start()
    with jax.named_scope("w_plane"):
        for copy in plane:
            copy.wait_recv()
    mean, m2 = merge(mean, m2, stat_a, PLANE, float(T))
    stat_m[0:1] = mean
    stat_m[1:2] = m2
    line = [
        remote(stat_m, stat_b.at[j], sb_send.at[j], sb_recv.at[j], line_peer(j))
        for j in range(1, NZ)
    ]
    for copy in line:
        copy.start()
    with jax.named_scope("w_line"):
        for copy in line:
            copy.wait_recv()
    mean, m2 = merge(mean, m2, stat_b, NZ, float(T * PLANE))
    var = m2 * (1.0 / (T * BLOCKS))
    factor = lax.rsqrt(var + 1e-5) * bng[...]

    outs = []
    for c in range(2):
        rs = slice(c * 256, (c + 1) * 256)
        a = after[rs]
        batched = ((a - mean) * factor + bns[...]).astype(BF16)
        hidden = jax.nn.gelu(mm(batched, wu[...]), approximate=True).astype(BF16)
        result[rs] = (a + mm(hidden, wd[...])).astype(BF16)
        copy = pltpu.make_async_copy(result.at[rs], out_hbm.at[rs], out_sem.at[c])
        copy.start()
        outs.append(copy)

    own_keys.wait_send()
    own_vals.wait_send()
    for copy in first + passed + second + plane + line:
        copy.wait_send()
    with jax.named_scope("w_outs"):
        for copy in outs:
            copy.wait()


def body(atoms, edge_mask, norm_gain, w_query, w_key, w_value, w_out, bn_gain, bn_shift, w_up, w_down):
    dma = pltpu.SemaphoreType.DMA
    args = (
        atoms, edge_mask, norm_gain.reshape(1, D), w_query, w_key, w_value, w_out,
        bn_gain.reshape(1, D), bn_shift.reshape(1, D), w_up, w_down,
    )
    vm = pltpu.VMEM
    return pl.pallas_call(
        kernel,
        out_shape=jax.ShapeDtypeStruct((T, D), BF16),
        in_specs=[pl.BlockSpec(memory_space=pl.ANY)] * len(args),
        out_specs=pl.BlockSpec(memory_space=pl.ANY),
        scratch_shapes=[
            vm((T, D), BF16), vm((SLABS, T, T), jnp.int32), vm((1, D), F32),
            vm((D, D), BF16), vm((D, D), BF16), vm((D, D), BF16), vm((D, D), BF16),
            vm((1, D), F32), vm((1, D), F32), vm((D, FF), BF16), vm((FF, D), BF16),
            vm((T, D), BF16), vm((3, T, D), BF16), vm((D, D), BF16), vm((D, D), BF16),
            vm((HEADS, 4 * HEAD_DIM, T), BF16), vm((SLABS, HEADS // 2, T, 128), BF16),
            vm((SLABS, HEADS, VROWS, T), BF16), vm((SLABS, T, T), F32),
            vm((T, T), F32), vm((T, T), F32),
            vm((8, T), F32), vm((8, T), F32), vm((HEADS, 8, T), F32), vm((HEADS, AROWS, T), F32),
            vm((D, T), BF16), vm((T, D), F32), vm((T, D), BF16),
            vm((2, D), F32), vm((PLANE, 2, D), F32), vm((2, D), F32), vm((NZ, 2, D), F32),
            dma((15,)), dma((2,)), dma((2,)), dma((2,)), dma((CHUNKS,)), dma((CHUNKS,)), dma((CHUNKS,)),
            dma((3, CHUNKS)), dma((PLANE,)), dma((PLANE,)), dma((NZ,)), dma((NZ,)),
        ],
        compiler_params=pltpu.CompilerParams(
            collective_id=0, has_side_effects=True, vmem_limit_bytes=63000 * 1024
        ),
    )(*args)


def solution(mesh):
    rows = P(("grp", "blk"), None)
    return jax.shard_map(
        body,
        mesh=mesh,
        in_specs=(rows, P(("grp", "blk"), None, None, None)) + (P(),) * 9,
        out_specs=rows,
        check_vma=False,
    )
```

```python
import functools
import math

import jax
import jax.numpy as jnp
from jax import lax
from jax.experimental import pallas as pl
from jax.experimental.pallas import tpu as pltpu
from jax.sharding import PartitionSpec as P

F32 = jnp.float32
BF16 = jnp.bfloat16
T = 512
D = 512
HEADS = 8
HEAD_DIM = 64
FF = 1024
SLABS = 5
OWN = 0
VROWS = 80
AROWS = 72
CHUNKS = 2
CROWS = T // CHUNKS
NEG = -1e30
SCALE = HEAD_DIM**-0.5 * math.log2(math.e)
NY, NZ, NX = 4, 8, 2
PLANE = NX * NY * 2
BLOCKS = PLANE * NZ


def mm(a, b):
    return jnp.dot(a, b, preferred_element_type=F32)


def mm_nt(a, b):
    return lax.dot_general(a, b, (((1,), (1,)), ((), ())), preferred_element_type=F32)


def kernel(
    atoms_hbm, mask_hbm, gain_hbm, wq_hbm, wk_hbm, wv_hbm, wo_hbm, bng_hbm, bns_hbm, wu_hbm, wd_hbm,
    out_hbm,
    atoms, mask, gain, wq, wk, wv, wo, bng, bns, wu, wd,
    nrm, recv, wqt, wvt, qz, keys, vals, bias, t0, t1, a0, a1, top, acc,
    mixed, after, result, stat, stat_a, stat_m, stat_b,
    load_sem, out_sem, own_send, own_recv, fst_send, fwd_send, snd_send, arrive,
    sa_send, sa_recv, sb_send, sb_recv,
):
    me = lax.axis_index("blk")
    core = lax.rem(me, 2)
    y = lax.rem(me // 2, NY)
    z = lax.rem(me // (2 * NY), NZ)
    xh = me // (2 * NY * NZ)
    sgn = 1 - 2 * core
    partner = me + sgn
    ahead = lax.rem(me + 2 * sgn + BLOCKS, BLOCKS)
    behind = lax.rem(me - 2 * sgn + BLOCKS, BLOCKS)
    place = xh * (NY * 2) + y * 2 + core

    def plane_peer(j):
        u = lax.rem(place + j, PLANE)
        return ((u // (NY * 2)) * NZ + z) * (NY * 2) + lax.rem(u, NY * 2)

    def line_peer(j):
        return (xh * NZ + lax.rem(z + j, NZ)) * (NY * 2) + y * 2 + core

    far_ahead = jnp.where(ahead // (2 * NY * NZ) == xh, 0, 1)

    swap = far_ahead * 3 * sgn
    offsets = [2, 2 + sgn, 2 + 2 * sgn - swap, 2 - sgn + swap, 2 - 2 * sgn]
    loads = [
        pltpu.make_async_copy(atoms_hbm, atoms, load_sem.at[11]),
        pltpu.make_async_copy(gain_hbm, gain, load_sem.at[12]),
        pltpu.make_async_copy(wq_hbm, wq, load_sem.at[0]),
        pltpu.make_async_copy(wk_hbm, wk, load_sem.at[1]),
        pltpu.make_async_copy(wv_hbm, wv, load_sem.at[2]),
    ]
    mask_loads = [
        pltpu.make_async_copy(mask_hbm.at[0, offsets[s]], mask.at[s], load_sem.at[3 + s])
        for s in range(SLABS)
    ]
    late = [
        pltpu.make_async_copy(wo_hbm, wo, load_sem.at[8]),
        pltpu.make_async_copy(bng_hbm, bng, load_sem.at[13]),
        pltpu.make_async_copy(bns_hbm, bns, load_sem.at[14]),
        pltpu.make_async_copy(wu_hbm, wu, load_sem.at[9]),
        pltpu.make_async_copy(wd_hbm, wd, load_sem.at[10]),
    ]
    for copy in loads + mask_loads + late:
        copy.start()

    barrier = pltpu.get_barrier_semaphore()
    peers = [partner, ahead, behind]
    peers += [plane_peer(j) for j in range(1, PLANE)]
    peers += [line_peer(j) for j in range(1, NZ)]
    for peer in peers:
        pl.semaphore_signal(
            barrier, inc=1, device_id={"blk": peer}, device_id_type=pl.DeviceIdType.MESH
        )

    def remote(src, dst, send, rec, device):
        return pltpu.make_async_remote_copy(
            src_ref=src, dst_ref=dst, send_sem=send, recv_sem=rec,
            device_id={"blk": device}, device_id_type=pl.DeviceIdType.MESH,
        )

    def rows(c):
        return pl.ds(c * CROWS, CROWS)

    own_keys = remote(keys.at[0], keys.at[1], own_send.at[0], own_recv.at[0], partner)
    own_vals = remote(vals.at[0], vals.at[1], own_send.at[1], own_recv.at[1], partner)
    first = [
        remote(nrm.at[rows(c)], recv.at[0, rows(c)], fst_send.at[c], arrive.at[0, c], behind)
        for c in range(CHUNKS)
    ]
    passed = [
        remote(recv.at[0, rows(c)], recv.at[1, rows(c)], fwd_send.at[c], arrive.at[1, c], partner)
        for c in range(CHUNKS)
    ]
    second = [
        remote(nrm.at[rows(c)], recv.at[2, rows(c)], snd_send.at[c], arrive.at[2, c], ahead)
        for c in range(CHUNKS)
    ]

    def arrived(slot, c):
        remote(recv.at[slot, rows(c)], recv.at[slot, rows(c)], fst_send.at[0], arrive.at[slot, c], partner).wait_recv()

    def start(copies):
        for copy in copies:
            copy.start()

    with jax.named_scope("w_atoms"):
        loads[0].wait()
        loads[1].wait()
    x = atoms[...].astype(F32)
    nrm[...] = (
        x * lax.rsqrt(jnp.mean(x * x, axis=-1, keepdims=True) + 1e-6) * gain[...]
    ).astype(BF16)
    with jax.named_scope("w_barrier"):
        pl.semaphore_wait(barrier, len(peers))
    start(first)

    with jax.named_scope("w_weights"):
        for copy in loads[2:]:
            copy.wait()
    wqt[...] = wq[...].T
    wvt[...] = wv[...].T

    def project(slot, features):
        k = mm(features, wk[...]).astype(BF16)
        for pair in range(HEADS // 2):
            keys[slot, pair] = k[:, pair * 128 : (pair + 1) * 128]
        v = mm_nt(wvt[...], features).astype(BF16)
        for h in range(HEADS):
            vals[slot, h, 0:HEAD_DIM] = v[h * HEAD_DIM : (h + 1) * HEAD_DIM]

    def make_bias(slot):
        mask_loads[slot].wait()
        for kc in range(T // 128):
            allowed = mask[slot, :, kc * 128 : (kc + 1) * 128] > 0
            if slot == 0:
                r = lax.broadcasted_iota(jnp.int32, (T, 128), 0)
                c = lax.broadcasted_iota(jnp.int32, (T, 128), 1) + kc * 128
                allowed = allowed | (r == c)
            bias[slot, kc * 128 : (kc + 1) * 128] = jnp.where(allowed, 0.0, NEG).astype(F32).T

    features = nrm[...]
    q = mm_nt(wqt[...], features).astype(BF16).astype(F32) * SCALE
    high = q.astype(BF16)
    low = (q - high.astype(F32)).astype(BF16)
    zero = jnp.zeros((HEAD_DIM, T), BF16)
    for h in range(HEADS):
        for i, piece in enumerate((high, low)):
            part = piece[h * HEAD_DIM : (h + 1) * HEAD_DIM]
            at = i * 2 * HEAD_DIM
            qz[h, at : at + HEAD_DIM] = part if h % 2 == 0 else zero
            qz[h, at + HEAD_DIM : at + 2 * HEAD_DIM] = zero if h % 2 == 0 else part
    for s in (0, 2, 3, 4):
        for h in range(HEADS):
            vals[s, h, HEAD_DIM:VROWS] = jnp.ones((VROWS - HEAD_DIM, T), BF16)
    project(0, features)
    own_keys.start()
    own_vals.start()
    with jax.named_scope("biases"):
        make_bias(0)
        make_bias(1)

    halves = (slice(0, 256), slice(256, 512))

    def score(slot, h, fresh):
        t, a = (t0, a0) if h % 2 == 0 else (t1, a1)
        for qs in halves:
            best = None
            for ks in halves:
                kp = keys[slot, h // 2, ks]
                s = mm(jnp.concatenate([kp, kp], axis=1), qz[h, :, qs]) + bias[slot, ks, qs]
                t[ks, qs] = s
                m = jnp.max(s.reshape(32, 8, 256), axis=0)
                best = m if best is None else jnp.maximum(best, m)
            best = jnp.max(best, axis=0, keepdims=True)
            if fresh:
                top[h, :, qs] = jnp.broadcast_to(best, (8, 256))
            else:
                old = top[h, :, qs]
                new = jnp.maximum(old, best)
                a[:, qs] = jnp.exp2(old - new)
                top[h, :, qs] = new

    def gather(slot, h, fresh):
        t, a = (t0, a0) if h % 2 == 0 else (t1, a1)
        for qs in halves:
            p = jnp.exp2(t[:, qs] - top[h, 0:1, qs]).astype(BF16)
            new = mm(vals[slot, h], p)[0:AROWS]
            if fresh:
                acc[h, :, qs] = new
            else:
                acc[h, :, qs] = acc[h, :, qs] * a[0:1, qs] + new

    def attend(slots):
        steps = [(slot, h, slot is OWN) for slot in slots for h in range(HEADS)]
        score(*steps[0])
        for i, step in enumerate(steps):
            if i + 1 < len(steps):
                score(*steps[i + 1])
            gather(*step)

    def fence():
        @pl.when(me < 0)
        def _():
            stat[...] = jnp.zeros_like(stat)

    fence()
    with jax.named_scope("attend0"):
        attend([OWN])
    fence()

    @pl.when(far_ahead == 0)
    def _():
        start(second)

    with jax.named_scope("w_partner"):
        own_keys.wait_recv()
        own_vals.wait_recv()
    fence()
    with jax.named_scope("attend1"):
        attend([1])

    @pl.when(far_ahead == 1)
    def _():
        start(second)

    make_bias(2)
    fence()
    with jax.named_scope("w_first"):
        for c in range(CHUNKS):
            arrived(far_ahead, c)

    @pl.when(far_ahead == 0)
    def _():
        start(passed)

    with jax.named_scope("project2"):
        project(2, recv[far_ahead])
    fence()
    with jax.named_scope("attend2"):
        attend([2])
    fence()
    make_bias(3)
    make_bias(4)
    fence()
    with jax.named_scope("w_passed"):
        for c in range(CHUNKS):
            arrived(1 - far_ahead, c)

    @pl.when(far_ahead == 1)
    def _():
        start(passed)

    with jax.named_scope("project3"):
        project(3, recv[1 - far_ahead])
    fence()
    with jax.named_scope("attend3"):
        attend([3])
    fence()
    with jax.named_scope("w_second"):
        for c in range(CHUNKS):
            arrived(2, c)
    with jax.named_scope("project4"):
        project(4, recv[2])
    fence()
    with jax.named_scope("attend4"):
        attend([4])
    fence()

    for h in range(HEADS):
        a = acc[h]
        mixed[h * HEAD_DIM : (h + 1) * HEAD_DIM] = (
            a[0:HEAD_DIM] * (1.0 / a[HEAD_DIM : HEAD_DIM + 1])
        ).astype(BF16)
    for copy in late:
        copy.wait()
    mix = mixed[...].T
    res = atoms[...].astype(F32) + mm(mix, wo[...])
    after[...] = res

    mean = jnp.sum(res, axis=0, keepdims=True) * (1.0 / T)
    dev = after[...] - mean
    m2 = jnp.sum(dev * dev, axis=0, keepdims=True)
    stat[0:1] = mean
    stat[1:2] = m2

    def merge(mean, m2, others, count, size):
        total = mean
        for j in range(1, count):
            total = total + others[j, 0:1]
        new = total * (1.0 / count)
        spread = (mean - new) * (mean - new)
        for j in range(1, count):
            d = others[j, 0:1] - new
            spread = spread + d * d
            m2 = m2 + others[j, 1:2]
        return new, m2 + spread * size

    plane = [
        remote(stat, stat_a.at[j], sa_send.at[j], sa_recv.at[j], plane_peer(j))
        for j in range(1, PLANE)
    ]
    for copy in plane:
        copy.start()
    with jax.named_scope("w_plane"):
        for copy in plane:
            copy.wait_recv()
    mean, m2 = merge(mean, m2, stat_a, PLANE, float(T))
    stat_m[0:1] = mean
    stat_m[1:2] = m2
    line = [
        remote(stat_m, stat_b.at[j], sb_send.at[j], sb_recv.at[j], line_peer(j))
        for j in range(1, NZ)
    ]
    for copy in line:
        copy.start()
    with jax.named_scope("w_line"):
        for copy in line:
            copy.wait_recv()
    mean, m2 = merge(mean, m2, stat_b, NZ, float(T * PLANE))
    var = m2 * (1.0 / (T * BLOCKS))
    factor = lax.rsqrt(var + 1e-5) * bng[...]

    outs = []
    for c in range(2):
        rs = slice(c * 256, (c + 1) * 256)
        a = after[rs]
        batched = ((a - mean) * factor + bns[...]).astype(BF16)
        hidden = jax.nn.gelu(mm(batched, wu[...]), approximate=True).astype(BF16)
        result[rs] = (a + mm(hidden, wd[...])).astype(BF16)
        copy = pltpu.make_async_copy(result.at[rs], out_hbm.at[rs], out_sem.at[c])
        copy.start()
        outs.append(copy)

    own_keys.wait_send()
    own_vals.wait_send()
    for copy in first + passed + second + plane + line:
        copy.wait_send()
    with jax.named_scope("w_outs"):
        for copy in outs:
            copy.wait()


def body(atoms, edge_mask, norm_gain, w_query, w_key, w_value, w_out, bn_gain, bn_shift, w_up, w_down):
    dma = pltpu.SemaphoreType.DMA
    args = (
        atoms, edge_mask, norm_gain.reshape(1, D), w_query, w_key, w_value, w_out,
        bn_gain.reshape(1, D), bn_shift.reshape(1, D), w_up, w_down,
    )
    vm = pltpu.VMEM
    return pl.pallas_call(
        kernel,
        out_shape=jax.ShapeDtypeStruct((T, D), BF16),
        in_specs=[pl.BlockSpec(memory_space=pl.ANY)] * len(args),
        out_specs=pl.BlockSpec(memory_space=pl.ANY),
        scratch_shapes=[
            vm((T, D), BF16), vm((SLABS, T, T), jnp.int32), vm((1, D), F32),
            vm((D, D), BF16), vm((D, D), BF16), vm((D, D), BF16), vm((D, D), BF16),
            vm((1, D), F32), vm((1, D), F32), vm((D, FF), BF16), vm((FF, D), BF16),
            vm((T, D), BF16), vm((3, T, D), BF16), vm((D, D), BF16), vm((D, D), BF16),
            vm((HEADS, 4 * HEAD_DIM, T), BF16), vm((SLABS, HEADS // 2, T, 128), BF16),
            vm((SLABS, HEADS, VROWS, T), BF16), vm((SLABS, T, T), F32),
            vm((T, T), F32), vm((T, T), F32),
            vm((8, T), F32), vm((8, T), F32), vm((HEADS, 8, T), F32), vm((HEADS, AROWS, T), F32),
            vm((D, T), BF16), vm((T, D), F32), vm((T, D), BF16),
            vm((2, D), F32), vm((PLANE, 2, D), F32), vm((2, D), F32), vm((NZ, 2, D), F32),
            dma((15,)), dma((2,)), dma((2,)), dma((2,)), dma((CHUNKS,)), dma((CHUNKS,)), dma((CHUNKS,)),
            dma((3, CHUNKS)), dma((PLANE,)), dma((PLANE,)), dma((NZ,)), dma((NZ,)),
        ],
        compiler_params=pltpu.CompilerParams(
            collective_id=0, has_side_effects=True, vmem_limit_bytes=63000 * 1024
        ),
    )(*args)


def solution(mesh):
    rows = P(("grp", "blk"), None)
    return jax.shard_map(
        body,
        mesh=mesh,
        in_specs=(rows, P(("grp", "blk"), None, None, None)) + (P(),) * 9,
        out_specs=rows,
        check_vma=False,
    )
```

```python
import functools
import math

import jax
import jax.numpy as jnp
from jax import lax
from jax.experimental import pallas as pl
from jax.experimental.pallas import tpu as pltpu
from jax.sharding import PartitionSpec as P

F32 = jnp.float32
BF16 = jnp.bfloat16
T = 512
D = 512
HEADS = 8
HEAD_DIM = 64
FF = 1024
SLABS = 5
OWN = 0
VROWS = 80
AROWS = 72
CHUNKS = 2
CROWS = T // CHUNKS
NEG = -1e30
SCALE = HEAD_DIM**-0.5 * math.log2(math.e)
NY, NZ, NX = 4, 8, 2
PLANE = NX * NY * 2
BLOCKS = PLANE * NZ


def mm(a, b):
    return jnp.dot(a, b, preferred_element_type=F32)


def mm_nt(a, b):
    return lax.dot_general(a, b, (((1,), (1,)), ((), ())), preferred_element_type=F32)


def kernel(
    atoms_hbm, mask_hbm, gain_hbm, wq_hbm, wk_hbm, wv_hbm, wo_hbm, bng_hbm, bns_hbm, wu_hbm, wd_hbm,
    out_hbm,
    atoms, mask, gain, wq, wk, wv, wo, bng, bns, wu, wd,
    nrm, recv, wqt, wvt, qz, keys, vals, bias, t0, t1, a0, a1, top, acc,
    mixed, after, result, stat, stat_a, stat_m, stat_b,
    load_sem, out_sem, own_send, own_recv, fst_send, fwd_send, snd_send, arrive,
    sa_send, sa_recv, sb_send, sb_recv,
):
    me = lax.axis_index("blk")
    core = lax.rem(me, 2)
    y = lax.rem(me // 2, NY)
    z = lax.rem(me // (2 * NY), NZ)
    xh = me // (2 * NY * NZ)
    sgn = 1 - 2 * core
    partner = me + sgn
    ahead = lax.rem(me + 2 * sgn + BLOCKS, BLOCKS)
    behind = lax.rem(me - 2 * sgn + BLOCKS, BLOCKS)
    place = xh * (NY * 2) + y * 2 + core

    def plane_peer(j):
        u = lax.rem(place + j, PLANE)
        return ((u // (NY * 2)) * NZ + z) * (NY * 2) + lax.rem(u, NY * 2)

    def line_peer(j):
        return (xh * NZ + lax.rem(z + j, NZ)) * (NY * 2) + y * 2 + core

    far_ahead = jnp.where(ahead // (2 * NY * NZ) == xh, 0, 1)

    swap = far_ahead * 3 * sgn
    offsets = [2, 2 + sgn, 2 + 2 * sgn - swap, 2 - sgn + swap, 2 - 2 * sgn]
    loads = [
        pltpu.make_async_copy(atoms_hbm, atoms, load_sem.at[11]),
        pltpu.make_async_copy(gain_hbm, gain, load_sem.at[12]),
        pltpu.make_async_copy(wq_hbm, wq, load_sem.at[0]),
        pltpu.make_async_copy(wk_hbm, wk, load_sem.at[1]),
        pltpu.make_async_copy(wv_hbm, wv, load_sem.at[2]),
    ]
    mask_loads = [
        pltpu.make_async_copy(mask_hbm.at[0, offsets[s]], mask.at[s], load_sem.at[3 + s])
        for s in range(SLABS)
    ]
    late = [
        pltpu.make_async_copy(wo_hbm, wo, load_sem.at[8]),
        pltpu.make_async_copy(bng_hbm, bng, load_sem.at[13]),
        pltpu.make_async_copy(bns_hbm, bns, load_sem.at[14]),
        pltpu.make_async_copy(wu_hbm, wu, load_sem.at[9]),
        pltpu.make_async_copy(wd_hbm, wd, load_sem.at[10]),
    ]
    for copy in loads + mask_loads + late:
        copy.start()

    barrier = pltpu.get_barrier_semaphore()
    peers = [partner, ahead, behind]
    peers += [plane_peer(j) for j in range(1, PLANE)]
    peers += [line_peer(j) for j in range(1, NZ)]
    for peer in peers:
        pl.semaphore_signal(
            barrier, inc=1, device_id={"blk": peer}, device_id_type=pl.DeviceIdType.MESH
        )

    def remote(src, dst, send, rec, device):
        return pltpu.make_async_remote_copy(
            src_ref=src, dst_ref=dst, send_sem=send, recv_sem=rec,
            device_id={"blk": device}, device_id_type=pl.DeviceIdType.MESH,
        )

    def rows(c):
        return pl.ds(c * CROWS, CROWS)

    own_keys = remote(keys.at[0], keys.at[1], own_send.at[0], own_recv.at[0], partner)
    own_vals = remote(vals.at[0], vals.at[1], own_send.at[1], own_recv.at[1], partner)
    first = [
        remote(nrm.at[rows(c)], recv.at[0, rows(c)], fst_send.at[c], arrive.at[0, c], behind)
        for c in range(CHUNKS)
    ]
    passed = [
        remote(recv.at[0, rows(c)], recv.at[1, rows(c)], fwd_send.at[c], arrive.at[1, c], partner)
        for c in range(CHUNKS)
    ]
    second = [
        remote(nrm.at[rows(c)], recv.at[2, rows(c)], snd_send.at[c], arrive.at[2, c], ahead)
        for c in range(CHUNKS)
    ]

    def arrived(slot, c):
        remote(recv.at[slot, rows(c)], recv.at[slot, rows(c)], fst_send.at[0], arrive.at[slot, c], partner).wait_recv()

    def start(copies):
        for copy in copies:
            copy.start()

    with jax.named_scope("w_atoms"):
        loads[0].wait()
        loads[1].wait()
    x = atoms[...].astype(F32)
    nrm[...] = (
        x * lax.rsqrt(jnp.mean(x * x, axis=-1, keepdims=True) + 1e-6) * gain[...]
    ).astype(BF16)
    with jax.named_scope("w_barrier"):
        pl.semaphore_wait(barrier, len(peers))
    start(first)

    with jax.named_scope("w_weights"):
        for copy in loads[2:]:
            copy.wait()
    wqt[...] = wq[...].T
    wvt[...] = wv[...].T

    def project(slot, features):
        k = mm(features, wk[...]).astype(BF16)
        for pair in range(HEADS // 2):
            keys[slot, pair] = k[:, pair * 128 : (pair + 1) * 128]
        v = mm_nt(wvt[...], features).astype(BF16)
        for h in range(HEADS):
            vals[slot, h, 0:HEAD_DIM] = v[h * HEAD_DIM : (h + 1) * HEAD_DIM]

    def make_bias(slot):
        mask_loads[slot].wait()
        for kc in range(T // 128):
            allowed = mask[slot, :, kc * 128 : (kc + 1) * 128] > 0
            if slot == 0:
                r = lax.broadcasted_iota(jnp.int32, (T, 128), 0)
                c = lax.broadcasted_iota(jnp.int32, (T, 128), 1) + kc * 128
                allowed = allowed | (r == c)
            bias[slot, kc * 128 : (kc + 1) * 128] = jnp.where(allowed, 0.0, NEG).astype(F32).T

    features = nrm[...]
    q = mm_nt(wqt[...], features).astype(BF16).astype(F32) * SCALE
    high = q.astype(BF16)
    low = (q - high.astype(F32)).astype(BF16)
    zero = jnp.zeros((HEAD_DIM, T), BF16)
    for h in range(HEADS):
        for i, piece in enumerate((high, low)):
            part = piece[h * HEAD_DIM : (h + 1) * HEAD_DIM]
            at = i * 2 * HEAD_DIM
            qz[h, at : at + HEAD_DIM] = part if h % 2 == 0 else zero
            qz[h, at + HEAD_DIM : at + 2 * HEAD_DIM] = zero if h % 2 == 0 else part
    for s in (0, 2, 3, 4):
        for h in range(HEADS):
            vals[s, h, HEAD_DIM:VROWS] = jnp.ones((VROWS - HEAD_DIM, T), BF16)
    project(0, features)
    own_keys.start()
    own_vals.start()
    with jax.named_scope("biases"):
        make_bias(0)
        make_bias(1)

    halves = (slice(0, 256), slice(256, 512))

    def score(slot, h, fresh):
        t, a = (t0, a0) if h % 2 == 0 else (t1, a1)
        for qs in halves:
            best = None
            for ks in halves:
                kp = keys[slot, h // 2, ks]
                s = mm(jnp.concatenate([kp, kp], axis=1), qz[h, :, qs]) + bias[slot, ks, qs]
                t[ks, qs] = s
                m = jnp.max(s.reshape(32, 8, 256), axis=0)
                best = m if best is None else jnp.maximum(best, m)
            best = jnp.max(best, axis=0, keepdims=True)
            if fresh:
                top[h, :, qs] = jnp.broadcast_to(best, (8, 256))
            else:
                old = top[h, :, qs]
                new = jnp.maximum(old, best)
                a[:, qs] = jnp.exp2(old - new)
                top[h, :, qs] = new

    def gather(slot, h, fresh):
        t, a = (t0, a0) if h % 2 == 0 else (t1, a1)
        for qs in halves:
            p = jnp.exp2(t[:, qs] - top[h, 0:1, qs]).astype(BF16)
            new = mm(vals[slot, h], p)[0:AROWS]
            if fresh:
                acc[h, :, qs] = new
            else:
                acc[h, :, qs] = acc[h, :, qs] * a[0:1, qs] + new

    def attend(slots):
        steps = [(slot, h, slot is OWN) for slot in slots for h in range(HEADS)]
        score(*steps[0])
        for i, step in enumerate(steps):
            if i + 1 < len(steps):
                score(*steps[i + 1])
            gather(*step)

    def fence():
        @pl.when(me < 0)
        def _():
            stat[...] = jnp.zeros_like(stat)

    fence()
    with jax.named_scope("attend0"):
        attend([OWN])
    fence()
    with jax.named_scope("w_partner"):
        own_keys.wait_recv()
        own_vals.wait_recv()
    fence()
    with jax.named_scope("attend1"):
        attend([1])
    fence()
    start(second)
    make_bias(2)
    fence()
    with jax.named_scope("w_first"):
        for c in range(CHUNKS):
            arrived(far_ahead, c)

    @pl.when(far_ahead == 0)
    def _():
        start(passed)

    with jax.named_scope("project2"):
        project(2, recv[far_ahead])
    fence()
    with jax.named_scope("attend2"):
        attend([2])
    fence()
    make_bias(3)
    make_bias(4)
    fence()
    with jax.named_scope("w_passed"):
        for c in range(CHUNKS):
            arrived(1 - far_ahead, c)

    @pl.when(far_ahead == 1)
    def _():
        start(passed)

    with jax.named_scope("project3"):
        project(3, recv[1 - far_ahead])
    fence()
    with jax.named_scope("attend3"):
        attend([3])
    fence()
    with jax.named_scope("w_second"):
        for c in range(CHUNKS):
            arrived(2, c)
    with jax.named_scope("project4"):
        project(4, recv[2])
    fence()
    with jax.named_scope("attend4"):
        attend([4])
    fence()

    for h in range(HEADS):
        a = acc[h]
        mixed[h * HEAD_DIM : (h + 1) * HEAD_DIM] = (
            a[0:HEAD_DIM] * (1.0 / a[HEAD_DIM : HEAD_DIM + 1])
        ).astype(BF16)
    for copy in late:
        copy.wait()
    mix = mixed[...].T
    res = atoms[...].astype(F32) + mm(mix, wo[...])
    after[...] = res

    mean = jnp.sum(res, axis=0, keepdims=True) * (1.0 / T)
    dev = after[...] - mean
    m2 = jnp.sum(dev * dev, axis=0, keepdims=True)
    stat[0:1] = mean
    stat[1:2] = m2

    def merge(mean, m2, others, count, size):
        total = mean
        for j in range(1, count):
            total = total + others[j, 0:1]
        new = total * (1.0 / count)
        spread = (mean - new) * (mean - new)
        for j in range(1, count):
            d = others[j, 0:1] - new
            spread = spread + d * d
            m2 = m2 + others[j, 1:2]
        return new, m2 + spread * size

    plane = [
        remote(stat, stat_a.at[j], sa_send.at[j], sa_recv.at[j], plane_peer(j))
        for j in range(1, PLANE)
    ]
    for copy in plane:
        copy.start()
    with jax.named_scope("w_plane"):
        for copy in plane:
            copy.wait_recv()
    mean, m2 = merge(mean, m2, stat_a, PLANE, float(T))
    stat_m[0:1] = mean
    stat_m[1:2] = m2
    line = [
        remote(stat_m, stat_b.at[j], sb_send.at[j], sb_recv.at[j], line_peer(j))
        for j in range(1, NZ)
    ]
    for copy in line:
        copy.start()
    with jax.named_scope("w_line"):
        for copy in line:
            copy.wait_recv()
    mean, m2 = merge(mean, m2, stat_b, NZ, float(T * PLANE))
    var = m2 * (1.0 / (T * BLOCKS))
    factor = lax.rsqrt(var + 1e-5) * bng[...]

    outs = []
    for c in range(2):
        rs = slice(c * 256, (c + 1) * 256)
        a = after[rs]
        batched = ((a - mean) * factor + bns[...]).astype(BF16)
        hidden = jax.nn.gelu(mm(batched, wu[...]), approximate=True).astype(BF16)
        result[rs] = (a + mm(hidden, wd[...])).astype(BF16)
        copy = pltpu.make_async_copy(result.at[rs], out_hbm.at[rs], out_sem.at[c])
        copy.start()
        outs.append(copy)

    own_keys.wait_send()
    own_vals.wait_send()
    for copy in first + passed + second + plane + line:
        copy.wait_send()
    with jax.named_scope("w_outs"):
        for copy in outs:
            copy.wait()


def body(atoms, edge_mask, norm_gain, w_query, w_key, w_value, w_out, bn_gain, bn_shift, w_up, w_down):
    dma = pltpu.SemaphoreType.DMA
    args = (
        atoms, edge_mask, norm_gain.reshape(1, D), w_query, w_key, w_value, w_out,
        bn_gain.reshape(1, D), bn_shift.reshape(1, D), w_up, w_down,
    )
    vm = pltpu.VMEM
    return pl.pallas_call(
        kernel,
        out_shape=jax.ShapeDtypeStruct((T, D), BF16),
        in_specs=[pl.BlockSpec(memory_space=pl.ANY)] * len(args),
        out_specs=pl.BlockSpec(memory_space=pl.ANY),
        scratch_shapes=[
            vm((T, D), BF16), vm((SLABS, T, T), jnp.int32), vm((1, D), F32),
            vm((D, D), BF16), vm((D, D), BF16), vm((D, D), BF16), vm((D, D), BF16),
            vm((1, D), F32), vm((1, D), F32), vm((D, FF), BF16), vm((FF, D), BF16),
            vm((T, D), BF16), vm((3, T, D), BF16), vm((D, D), BF16), vm((D, D), BF16),
            vm((HEADS, 4 * HEAD_DIM, T), BF16), vm((SLABS, HEADS // 2, T, 128), BF16),
            vm((SLABS, HEADS, VROWS, T), BF16), vm((SLABS, T, T), F32),
            vm((T, T), F32), vm((T, T), F32),
            vm((8, T), F32), vm((8, T), F32), vm((HEADS, 8, T), F32), vm((HEADS, AROWS, T), F32),
            vm((D, T), BF16), vm((T, D), F32), vm((T, D), BF16),
            vm((2, D), F32), vm((PLANE, 2, D), F32), vm((2, D), F32), vm((NZ, 2, D), F32),
            dma((15,)), dma((2,)), dma((2,)), dma((2,)), dma((CHUNKS,)), dma((CHUNKS,)), dma((CHUNKS,)),
            dma((3, CHUNKS)), dma((PLANE,)), dma((PLANE,)), dma((NZ,)), dma((NZ,)),
        ],
        compiler_params=pltpu.CompilerParams(
            collective_id=0, has_side_effects=True, vmem_limit_bytes=63000 * 1024
        ),
    )(*args)


def solution(mesh):
    rows = P(("grp", "blk"), None)
    return jax.shard_map(
        body,
        mesh=mesh,
        in_specs=(rows, P(("grp", "blk"), None, None, None)) + (P(),) * 9,
        out_specs=rows,
        check_vma=False,
    )
```
